32 devices in a mesh: frames: 16 (over z, x, core), groups: 2 (over y).
Axes of the slice: x: 2, y: 2, z: 4, core: 2. Of those that a mesh axis runs over, the one named last changes fastest.
Arguments:
- parents: bfloat16 [8, 2048, 1024], P('groups', 'frames'), may hold values from -6 to 6
- children: bfloat16 [8, 2048, 1024], P('groups', 'frames'), may hold values from -6 to 6
- child_counts: int32 [8, 16], P('groups'), may hold values from 32 to 128
- out_grad: bfloat16 [8, 2048, 1024], P('groups', 'frames'), may hold values from -6 to 6
- child_gain: bfloat16 [1024], replicated, may hold values from 0.5 to 1.5
- cross_gain: bfloat16 [1024], replicated, may hold values from 0.5 to 1.5
- cross_query: bfloat16 [1024, 1024], replicated, may hold values from -0.1875 to 0.1875
- cross_keyval: bfloat16 [1024, 2048], replicated, may hold values from -0.1875 to 0.1875
- cross_output: bfloat16 [1024, 1024], replicated, may hold values from -0.75 to 0.75
- self_gain: bfloat16 [1024], replicated, may hold values from 0.5 to 1.5
- self_project: bfloat16 [1024, 3072], replicated, may hold values from -0.1875 to 0.1875
- self_output: bfloat16 [1024, 1024], replicated, may hold values from -0.75 to 0.75
- mlp_gain: bfloat16 [1024], replicated, may hold values from 0.5 to 1.5
- mlp_up: bfloat16 [1024, 4096], replicated, may hold values from -0.1875 to 0.1875
- mlp_down: bfloat16 [4096, 1024], replicated, may hold values from -0.09375 to 0.09375
Outputs:
- top_latents: bfloat16 [8, 2048, 1024], P('groups', 'frames')
- grad_parents: float32 [8, 2048, 1024], P('groups', 'frames')
- grad_children: float32 [8, 2048, 1024], P('groups', 'frames')
- grad_child_gain: float32 [1024], P('frames')
- grad_cross_gain: float32 [1024], P('frames')
- grad_cross_query: float32 [1024, 1024], P('frames')
- grad_cross_keyval: float32 [1024, 2048], P('frames')
- grad_cross_output: float32 [1024, 1024], P('frames')
- grad_self_gain: float32 [1024], P('frames')
- grad_self_project: float32 [1024, 3072], P('frames')
- grad_self_output: float32 [1024, 1024], P('frames')
- grad_mlp_gain: float32 [1024], P('frames')
- grad_mlp_up: float32 [1024, 4096], P('frames')
- grad_mlp_down: float32 [4096, 1024], P('frames')
The draws below stay inside these ranges and needn't reach their ends.
Inputs may be any that keep to these rules, and one draw needn't show every extreme that they name: child_counts[b, f] is the number of leading valid child latents of clip b at frame f; the rest are padding.
All inputs are finite; a program needn't handle non-finite values.
Results may differ from the reference program's by a relative error of at most 0.025.
Values may be sent and summed in bfloat16 or wider, within the bound.
A program may use at most 256 MiB of HBM per device.

```python
import jax
import jax.numpy as jnp
from jax import lax

HEADS = 8
HEAD_DIM = 128
D = 1024
FF = 4096
HALF = 128
CHILD = 128
LEVEL = 1
BATCH = 8
SPAN = 2048
CSPAN = 2048
N_FRAMES = 16


def touch_ends(values, key, least, largest):
    index_at = [jax.random.randint(jax.random.fold_in(key, axis), (), 0, length) for axis, length in enumerate(values.shape)]
    main_axis = values.shape.index(max(values.shape))
    next_to = index_at[:main_axis] + [(index_at[main_axis] + 1) % values.shape[main_axis]] + index_at[main_axis + 1:]
    return values.at[tuple(index_at)].set(least).at[tuple(next_to)].set(largest)


def shard_levels(own_key, shape, split, least, largest):
    level = 1.0
    for position, blocks in split:
        draws = jax.random.uniform(jax.random.fold_in(jax.random.fold_in(own_key, 6), position), (blocks,), jnp.float32, least / len(split), largest / len(split))
        level = level * jnp.repeat(jnp.exp(draws), shape[position] // blocks).reshape((-1,) + (1,) * (len(shape) - 1 - position))
    return level


def gaussian(own_key, extent, scale, limit, pieces=(), kind=jnp.bfloat16):
    loudness = shard_levels(own_key, extent, pieces, -0.22, 0.18) if pieces else 1.0
    values = jax.random.normal(own_key, extent, jnp.float32) * scale * loudness
    return jnp.minimum(jnp.maximum(values, -limit), limit).astype(kind)


def setup_inputs(seed: int = 0) -> dict:
    keys = jax.random.split(jax.random.key(seed), 16)
    return {
        "parents": gaussian(keys[0], (BATCH, SPAN, D), 1.0, 6.0, ((0, 2), (1, 16))),
        "children": gaussian(keys[1], (BATCH, CSPAN, D), 1.0, 6.0, ((0, 2), (1, 16))),
        "child_counts": touch_ends(jax.random.randint(keys[2], (BATCH, N_FRAMES), max(1, CHILD // 4), CHILD + 1), jax.random.fold_in(keys[2], 1), max(1, CHILD // 4), CHILD).astype(jnp.int32),
        "out_grad": gaussian(keys[3], (BATCH, SPAN, D), 1.0, 6.0, ((0, 2), (1, 16))),
        "child_gain": jnp.clip(1.0 + 0.1 * jax.random.normal(keys[4], (D,), jnp.float32), 0.5, 1.5).astype(jnp.bfloat16),
        "cross_gain": jnp.clip(1.0 + 0.1 * jax.random.normal(keys[5], (D,), jnp.float32), 0.5, 1.5).astype(jnp.bfloat16),
        "cross_query": gaussian(keys[6], (D, D), D ** -0.5, 0.1875),
        "cross_keyval": gaussian(keys[7], (D, 2 * D), D ** -0.5, 0.1875),
        "cross_output": gaussian(keys[8], (D, D), (D // 16) ** -0.5, 0.75),
        "self_gain": jnp.clip(1.0 + 0.1 * jax.random.normal(keys[9], (D,), jnp.float32), 0.5, 1.5).astype(jnp.bfloat16),
        "self_project": gaussian(keys[10], (D, 3 * D), D ** -0.5, 0.1875),
        "self_output": gaussian(keys[11], (D, D), (D // 16) ** -0.5, 0.75),
        "mlp_gain": jnp.clip(1.0 + 0.1 * jax.random.normal(keys[12], (D,), jnp.float32), 0.5, 1.5).astype(jnp.bfloat16),
        "mlp_up": gaussian(keys[13], (D, FF), D ** -0.5, 0.1875),
        "mlp_down": gaussian(keys[14], (FF, D), FF ** -0.5, 0.09375),
    }


@jax.custom_vjp
def low(v):
    return lax.optimization_barrier(v.astype(jnp.bfloat16)).astype(jnp.float32)

@jax.custom_vjp
def low_back(v):
    return v

def low_keep(v):
    return (low(v), None)

def low_pass(kept, grad):
    return (grad,)

def back_keep(v):
    return (v, None)

def back_low(kept, grad):
    return (low(grad),)
low.defvjp(low_keep, low_pass)
low_back.defvjp(back_keep, back_low)

def layer_norm(values, gain):
    average = lax.optimization_barrier(jnp.mean(values, axis=-1, keepdims=True))
    centred = values - average
    spread = lax.optimization_barrier(jnp.mean(centred * centred, axis=-1, keepdims=True))
    return centred * lax.rsqrt(spread + 1e-05) * gain

def product(left, right):
    return jnp.dot(left, right, precision=lax.Precision.HIGHEST, preferred_element_type=jnp.float32)

def attend(queries, key_rows, value_rows, key_valid):
    query_count = queries.shape[0]
    key_count = key_rows.shape[0]
    query_heads = queries.reshape(query_count, HEADS, HEAD_DIM)
    key_heads = key_rows.reshape(key_count, HEADS, HEAD_DIM)
    value_heads = value_rows.reshape(key_count, HEADS, HEAD_DIM)
    scores = jnp.einsum('qhd,khd->hqk', query_heads, key_heads, precision=lax.Precision.HIGHEST) * HEAD_DIM ** (-0.5)
    scores = low_back(scores)
    scores = jnp.where(key_valid[None, None, :], scores, -1e+30)
    weights = jax.nn.softmax(scores, axis=-1)
    mixture = jnp.einsum('hqk,khd->qhd', low(weights), value_heads, precision=lax.Precision.HIGHEST)
    return mixture.reshape(query_count, HEADS * HEAD_DIM)

def node_block(node_rows, child_rows, key_valid, params):
    child_gain, cross_gain, cross_query, cross_keyval, cross_output, self_gain, self_project, self_output, mlp_gain, mlp_up, mlp_down = params
    features = node_rows.shape[1]
    child_in = low(layer_norm(child_rows, child_gain))
    keyval = low(low_back(product(child_in, cross_keyval)))
    cross_in = low(layer_norm(node_rows, cross_gain))
    queries = low(low_back(product(cross_in, cross_query)))
    attended = low(low_back(attend(queries, keyval[:, :features], keyval[:, features:], key_valid)))
    after_cross = node_rows + low_back(product(attended, cross_output))
    self_in = low(layer_norm(after_cross, self_gain))
    projected = low(low_back(product(self_in, self_project)))
    everyone = jnp.ones((node_rows.shape[0],), jnp.int32) > 0
    self_mix = low(low_back(attend(projected[:, :features], projected[:, features:2 * features], projected[:, 2 * features:], everyone)))
    after_self = after_cross + low_back(product(self_mix, self_output))
    mlp_in = low(layer_norm(after_self, mlp_gain))
    hidden = low_back(product(mlp_in, mlp_up))
    activated = low(jax.nn.gelu(hidden, approximate=False))
    return after_self + low_back(product(activated, mlp_down))

def to_nodes(array, row_count):
    batch_size = array.shape[0]
    features = array.shape[-1]
    distance = 2 ** LEVEL
    shaped = array.reshape(batch_size, N_FRAMES // (2 * distance), 2, distance, row_count, features)
    return shaped.transpose(0, 1, 3, 2, 4, 5).reshape(-1, 2 * row_count, features)

def from_nodes(node_array, batch_size, row_count):
    features = node_array.shape[-1]
    distance = 2 ** LEVEL
    shaped = node_array.reshape(batch_size, N_FRAMES // (2 * distance), distance, 2, row_count, features)
    return shaped.transpose(0, 1, 3, 2, 4, 5).reshape(batch_size, N_FRAMES * row_count, features)

def reference(parents, children, child_counts, out_grad, child_gain, cross_gain, cross_query, cross_keyval, cross_output, self_gain, self_project, self_output, mlp_gain, mlp_up, mlp_down):
    distance = 2 ** LEVEL
    batch_size = parents.shape[0]
    counts_shaped = child_counts.reshape(batch_size, N_FRAMES // (2 * distance), 2, distance)
    node_counts = counts_shaped.transpose(0, 1, 3, 2).reshape(-1, 2)
    positions = jnp.arange(CHILD, dtype=jnp.int32)
    key_valid = (positions[None, None, :] < node_counts[:, :, None]).reshape(-1, 2 * CHILD)
    floats = [array.astype(jnp.float32) for array in (parents, children, child_gain, cross_gain, cross_query, cross_keyval, cross_output, self_gain, self_project, self_output, mlp_gain, mlp_up, mlp_down)]

    def forward(parent_rows, child_latents, *params):
        node_rows = to_nodes(parent_rows, HALF)
        child_rows = to_nodes(child_latents, CHILD)

        def one_node(packed):
            return node_block(packed[0], packed[1], packed[2], params)
        result = lax.map(jax.checkpoint(one_node), (node_rows, child_rows, key_valid))
        return from_nodes(result, batch_size, HALF)
    latent_out, pullback = jax.vjp(forward, *floats)
    gradients = pullback(out_grad.astype(jnp.float32))
    return (latent_out.astype(jnp.bfloat16), gradients[0], gradients[1], gradients[2], gradients[3], gradients[4], gradients[5], gradients[6], gradients[7], gradients[8], gradients[9], gradients[10], gradients[11], gradients[12])
```

```python
from functools import partial

import jax
import jax.numpy as jnp
from jax import lax
from jax.experimental import pallas as pl
from jax.experimental.pallas import tpu as pltpu
from jax.sharding import PartitionSpec as P

HEADS = 8
HEAD_DIM = 128
LEVEL = 1
SCALE = HEAD_DIM ** (-0.5)
LOW = jnp.bfloat16
WIDE = jnp.float32
MIB = 1 << 20


def bit_of(value, place):
    return (value // (1 << place)) % 2


def flipped(value, place):
    return value + (1 << place) - (2 << place) * bit_of(value, place)


def xor_static(constant, value, places):
    total = 0
    for place in range(places):
        bit = bit_of(value, place)
        total = total + ((1 - bit) if (constant >> place) & 1 else bit) * (1 << place)
    return total


def swapped(value, axis, place):
    mask = 1 << place
    return lax.ppermute(value, axis, [(s, s ^ mask) for s in range(lax.axis_size(axis))])


def to_nodes(value):
    half = value.shape[0] // 2
    side = bit_of(lax.axis_index("frames"), LEVEL)
    kept = lax.dynamic_slice_in_dim(value, side * half, half, 0)
    sent = lax.dynamic_slice_in_dim(value, (1 - side) * half, half, 0)
    return kept, swapped(sent, "frames", LEVEL)


def from_nodes(own, back):
    side = bit_of(lax.axis_index("frames"), LEVEL)
    first = jnp.concatenate([own, back], axis=0)
    second = jnp.concatenate([back, own], axis=0)
    return jnp.where(side == 0, first, second)


def layer_norm(values, gain):
    average = jnp.mean(values, axis=-1, keepdims=True)
    centred = values - average
    spread = jnp.mean(centred * centred, axis=-1, keepdims=True)
    return centred * lax.rsqrt(spread + 1e-05) * gain


def norm_back(values, gain, grad_out):
    average = jnp.mean(values, axis=-1, keepdims=True)
    centred = values - average
    spread = jnp.mean(centred * centred, axis=-1, keepdims=True)
    inverse = lax.rsqrt(spread + 1e-05)
    normed = centred * inverse
    scaled = grad_out * gain
    grad = inverse * (
        scaled
        - jnp.mean(scaled, axis=-1, keepdims=True)
        - normed * jnp.mean(scaled * normed, axis=-1, keepdims=True)
    )
    return grad, jnp.sum(grad_out * normed, axis=0)


def matmul(left, right):
    return jnp.dot(left, right, preferred_element_type=WIDE)


def product_back(grad_rows, weight):
    return lax.dot_general(
        grad_rows, weight, (((1,), (1,)), ((), ())), preferred_element_type=WIDE
    )


def weight_grad(inputs, grad_rows):
    return lax.dot_general(
        inputs, grad_rows, (((0,), (0,)), ((), ())), preferred_element_type=WIDE
    )


def dot_nt(left, right):
    return lax.dot_general(left, right, (((1,), (1,)), ((), ())), preferred_element_type=WIDE)


def dot_tn(left, right):
    return lax.dot_general(left, right, (((0,), (0,)), ((), ())), preferred_element_type=WIDE)


def node_rows(ref, head):
    block = ref[:, 0, :, head * HEAD_DIM : (head + 1) * HEAD_DIM]
    return block.reshape(block.shape[0] * block.shape[1], HEAD_DIM)


def valid_keys(count_ref, rows, shape, axis):
    node = pl.program_id(0)
    key = lax.broadcasted_iota(jnp.int32, shape, axis)
    first, second = count_ref[0, node], count_ref[1, node]
    return key < jnp.where(key < rows, first, second + rows)


def attend_kernel(masked, count_ref, q_ref, k_ref, v_ref, out_ref):
    heads = q_ref.shape[3] // HEAD_DIM
    rows = q_ref.shape[2]
    for head in range(heads):
        q, k, v = (node_rows(ref, head) for ref in (q_ref, k_ref, v_ref))
        scores = dot_nt(q, k) * SCALE
        if masked:
            scores = jnp.where(valid_keys(count_ref, rows, scores.shape, 1), scores, -1e30)
        top = jnp.max(scores, axis=1, keepdims=True)
        raised = jnp.exp(scores - top)
        weights = raised / jnp.sum(raised, axis=1, keepdims=True)
        mixed = jnp.dot(weights.astype(LOW), v, preferred_element_type=WIDE)
        out_ref[:, 0, :, head * HEAD_DIM : (head + 1) * HEAD_DIM] = mixed.astype(LOW).reshape(
            2, rows, HEAD_DIM
        )


def attend_back_kernel(masked, count_ref, q_ref, k_ref, v_ref, grad_ref, *outs):
    heads = q_ref.shape[3] // HEAD_DIM
    rows = q_ref.shape[2]
    wide = heads * HEAD_DIM
    places = [(outs[0], 0), (outs[-1], wide if len(outs) == 1 else 0)]
    places.append((outs[-1], places[1][1] + wide))
    for head in range(heads):
        q, k, v, grad = (node_rows(ref, head) for ref in (q_ref, k_ref, v_ref, grad_ref))
        scores = dot_nt(k, q) * SCALE
        if masked:
            scores = jnp.where(valid_keys(count_ref, rows, scores.shape, 0), scores, -1e30)
        top = jnp.max(scores, axis=0, keepdims=True)
        raised = jnp.exp(scores - top)
        weights = raised / jnp.sum(raised, axis=0, keepdims=True)
        grad_weights = dot_nt(v, grad)
        inner = jnp.sum(weights * grad_weights, axis=0, keepdims=True)
        grad_scores = (weights * (grad_weights - inner)).astype(LOW)
        results = (
            dot_tn(grad_scores, k) * SCALE,
            jnp.dot(grad_scores, q, preferred_element_type=WIDE) * SCALE,
            jnp.dot(weights.astype(LOW), grad, preferred_element_type=WIDE),
        )
        for (ref, start), result in zip(places, results):
            start = start + head * HEAD_DIM
            ref[:, 0, :, start : start + HEAD_DIM] = result.astype(LOW).reshape(2, rows, HEAD_DIM)


def column_block(rows, width, column):
    return pl.BlockSpec((2, 1, rows, width), lambda node, *_: (0, node, 0, column))


def attend(counts, queries, keyval, key_column, masked):
    _, nodes, rows, _ = queries.shape
    features = HEADS * HEAD_DIM
    spec = pltpu.PrefetchScalarGridSpec(
        num_scalar_prefetch=1,
        grid=(nodes,),
        in_specs=[column_block(rows, features, c) for c in (0, key_column, key_column + 1)],
        out_specs=column_block(rows, features, 0),
    )
    flops = 4 * nodes * HEADS * (2 * rows) ** 2 * HEAD_DIM
    return pl.pallas_call(
        partial(attend_kernel, masked),
        grid_spec=spec,
        out_shape=jax.ShapeDtypeStruct((2, nodes, rows, features), LOW),
        cost_estimate=pl.CostEstimate(
            flops=flops, bytes_accessed=8 * 2 * nodes * rows * features, transcendentals=flops // 512
        ),
        name="attend",
    )(counts, queries, keyval, keyval)


def attend_back(counts, queries, keyval, key_column, masked, grad_mix):
    _, nodes, rows, _ = queries.shape
    features = HEADS * HEAD_DIM
    widths = (3 * features,) if key_column == 1 else (features, 2 * features)
    spec = pltpu.PrefetchScalarGridSpec(
        num_scalar_prefetch=1,
        grid=(nodes,),
        in_specs=[column_block(rows, features, c) for c in (0, key_column, key_column + 1, 0)],
        out_specs=[column_block(rows, width, 0) for width in widths],
    )
    flops = 10 * nodes * HEADS * (2 * rows) ** 2 * HEAD_DIM
    return pl.pallas_call(
        partial(attend_back_kernel, masked),
        grid_spec=spec,
        out_shape=[jax.ShapeDtypeStruct((2, nodes, rows, width), LOW) for width in widths],
        cost_estimate=pl.CostEstimate(
            flops=flops, bytes_accessed=14 * 2 * nodes * rows * features, transcendentals=flops // 1280
        ),
        name="attend_back",
    )(counts, queries, keyval, keyval, grad_mix)


def feed_kernel(in_ref, grad_ref, up_ref, down_ref, act_ref, grad_hidden_ref, out_ref, grad_in_ref):
    step = pl.program_id(0)

    @pl.when(step == 0)
    def _():
        out_ref[...] = jnp.zeros_like(out_ref)
        grad_in_ref[...] = jnp.zeros_like(grad_in_ref)

    rows = in_ref.shape[0]
    part = rows // 2
    for start in range(0, rows, part):
        here = pl.ds(start, part)
        hidden = jnp.dot(in_ref[here, :], up_ref[...], preferred_element_type=WIDE)
        grad_act = dot_nt(grad_ref[here, :], down_ref[...])
        normal = 0.5 * (1.0 + lax.erf(hidden * 0.7071067811865476))
        density = jnp.exp(-0.5 * hidden * hidden) * 0.3989422804014327
        act = (hidden * normal).astype(LOW)
        grad_hidden = (grad_act * (normal + hidden * density)).astype(LOW)
        act_ref[here, :] = act
        grad_hidden_ref[here, :] = grad_hidden
        out_ref[here, :] += jnp.dot(act, down_ref[...], preferred_element_type=WIDE)
        grad_in_ref[here, :] += dot_nt(grad_hidden, up_ref[...])


def feed(mlp_in, grad_low, mlp_up, mlp_down):
    rows, features = mlp_in.shape
    hidden = mlp_up.shape[1]
    tile = min(512, hidden)
    whole = pl.BlockSpec((rows, features), lambda i: (0, 0))
    return pl.pallas_call(
        feed_kernel,
        grid=(hidden // tile,),
        in_specs=[
            whole,
            whole,
            pl.BlockSpec((features, tile), lambda i: (0, i)),
            pl.BlockSpec((tile, features), lambda i: (i, 0)),
        ],
        out_specs=[
            pl.BlockSpec((rows, tile), lambda i: (0, i)),
            pl.BlockSpec((rows, tile), lambda i: (0, i)),
            whole,
            whole,
        ],
        out_shape=[
            jax.ShapeDtypeStruct((rows, hidden), LOW),
            jax.ShapeDtypeStruct((rows, hidden), LOW),
            jax.ShapeDtypeStruct((rows, features), WIDE),
            jax.ShapeDtypeStruct((rows, features), WIDE),
        ],
        compiler_params=pltpu.CompilerParams(vmem_limit_bytes=40 * MIB),
        cost_estimate=pl.CostEstimate(
            flops=8 * rows * features * hidden,
            bytes_accessed=4 * features * hidden + 12 * rows * hidden,
            transcendentals=2 * rows * hidden,
        ),
        name="feed",
    )(mlp_in, grad_low, mlp_up, mlp_down)


CHUNK = 1024
SHARES = (512, 256, 256)


class Plan:
    def __init__(self, frames, groups, inner):
        self.frames, self.groups = frames, groups
        self.places = frames.bit_length() - 1
        self.group_places = groups.bit_length() - 1
        self.rows = inner // frames
        self.split = groups == 2 and self.rows % 32 == 0
        self.part = self.rows // 2 if self.split else self.rows
        near, far = [("f", 1)], [("f", d) for d in range(2, self.places)]
        if self.split:
            cut, join, add = [("cut", 0)], [("join", 0)], [("add", 0)]
            self.orders = [near + cut + far + join, cut + far + near + join, far + near + add]
        else:
            add = [("add", e) for e in range(self.group_places)]
            self.orders = [near + far + add, far + near + add, far + near + add]
        self.depth = max(len(order) for order in self.orders)
        starts = [0]
        for share in SHARES:
            starts.append(starts[-1] + share)
        self.columns = [(starts[i], SHARES[i]) for i in range(len(SHARES))]
        self.steps = []
        for (start, width), order in zip(self.columns, self.orders):
            fixed, size, steps = {}, self.rows, []
            for kind, place in order:
                free = [d for d in range(1, self.places) if d not in fixed]
                if kind == "f":
                    send, keep = dict(fixed), dict(fixed)
                    send[place], keep[place] = 1, 0
                    send_rows = keep_rows = (0, size)
                    fixed[place] = 0
                    free.remove(place)
                elif kind == "cut":
                    send = keep = dict(fixed)
                    send_rows, keep_rows = (self.part, self.part), (0, self.part)
                    size = self.part
                else:
                    send = keep = dict(fixed)
                    send_rows = keep_rows = (0, size)
                shape = (2,) * len(free) + (send_rows[1], width)
                steps.append((kind, place, send, send_rows, keep, keep_rows, shape))
            self.steps.append(steps)

    def index(self, slot, fixed, rows, columns):
        middle = [fixed.get(d, slice(None)) for d in reversed(range(1, self.places))]
        return tuple([slot] + middle + [pl.ds(*rows), pl.ds(*columns)])


def reduce_kernel(plan, sources, slots, n_in, *refs):
    ins, out_ref, rest = refs[:n_in], refs[n_in], refs[n_in + 1 :]
    raw, grad, turned, sent, held, core_in, load_sem, core_send, core_recv, send_sem, recv_sem = rest[:11]
    lands = rest[11:]
    chunks = len(sources)
    frame, group = lax.axis_index("frames"), lax.axis_index("groups")
    rows, part, places = plan.rows, plan.part, plan.places
    halves = rows // part
    blocks = plan.frames // 2

    ids, count = {}, 0
    for i, steps in enumerate(plan.steps):
        for k in range(len(steps)):
            ids[i, k] = count
            count += 1

    def partner(kind, place):
        if kind == "f":
            return {"frames": flipped(frame, place), "groups": group}
        return {"frames": frame, "groups": flipped(group, place)}

    barrier = pltpu.get_barrier_semaphore()
    everyone = [partner("f", d) for d in range(places)] + [
        partner("g", e) for e in range(plan.group_places)
    ]
    for device in everyone:
        pl.semaphore_signal(barrier, inc=1, device_id=device, device_id_type=pl.DeviceIdType.MESH)
    pl.semaphore_wait(barrier, len(everyone))

    def core_copy(u):
        s = u % 2
        return pltpu.make_async_remote_copy(
            src_ref=sent.at[s],
            dst_ref=core_in.at[s],
            send_sem=core_send.at[s],
            recv_sem=core_recv.at[s],
            device_id=partner("f", 0),
            device_id_type=pl.DeviceIdType.MESH,
        )

    def step_copy(i, k, u):
        kind, place, send, send_rows, _, _, _ = plan.steps[i][k]
        s = u % 2
        return pltpu.make_async_remote_copy(
            src_ref=held.at[plan.index(u % slots, send, send_rows, plan.columns[i])],
            dst_ref=lands[ids[i, k]].at[s],
            send_sem=send_sem.at[ids[i, k], s],
            recv_sem=recv_sem.at[ids[i, k], s],
            device_id=partner(kind, place),
            device_id_type=pl.DeviceIdType.MESH,
        )

    def loads(t, which):
        left, right, column = sources[which]
        s = t % 2
        return (
            pltpu.make_async_copy(ins[left], raw.at[s], load_sem.at[0, s]),
            pltpu.make_async_copy(
                ins[right].at[:, column : column + CHUNK], grad.at[s], load_sem.at[1, s]
            ),
        )

    def row_place(half):
        if halves == 1:
            return 0
        place = bit_of(group, 0)
        return ((1 - place) if half else place) * part

    def finish(i, k, u):
        kind, _, _, _, keep, keep_rows, _ = plan.steps[i][k]
        start, width = plan.columns[i]
        land = lands[ids[i, k]]
        s = u % 2
        if kind == "join":
            mine = held[plan.index(u % slots, keep, (0, part), plan.columns[i])]
            other = land[s]
            for half, value in ((0, mine), (1, other)):
                at = pl.multiple_of(row_place(half), part)
                out_ref[u, pl.ds(at, part), pl.ds(start, width)] = value.astype(WIDE)
        else:
            for half in range(halves):
                source = (halves - 1 - half) * part
                mine = held[plan.index(u % slots, keep, (half * part, part), plan.columns[i])]
                other = land[s, pl.ds(source, part), :]
                at = pl.multiple_of(row_place(half), part)
                out_ref[u, pl.ds(at, part), pl.ds(start, width)] = mine.astype(WIDE) + other.astype(WIDE)

    def advance(i, k, u):
        step_copy(i, k, u).wait()
        if k == len(plan.steps[i]) - 1:
            finish(i, k, u)
            return
        _, _, _, _, keep, keep_rows, _ = plan.steps[i][k]
        at = plan.index(u % slots, keep, keep_rows, plan.columns[i])
        held[at] = held[at] + lands[ids[i, k]][u % 2]
        step_copy(i, k + 1, u).start()

    def turn(s):
        width = 128
        for tile in range(raw.shape[2] // width):
            value = raw[s, :, tile * width : (tile + 1) * width].T
            for piece in range(width // part):
                at = tile * (width // part) + piece
                block, half = at // halves, at % halves
                where = xor_static(block, frame, places)
                row = (where // 2) * rows
                if halves > 1:
                    row = row + xor_static(half, group, 1) * part
                row = pl.multiple_of(row, part)
                turned[where % 2, pl.ds(row, part), :] = value[piece * part : (piece + 1) * part, :]

    def make(t):
        s = t % 2
        for copy in loads(t, 0):
            copy.wait()
        for which in range(1, chunks):

            @pl.when(t + 1 == which)
            def _():
                for copy in loads(t + 1, which):
                    copy.start()

        turn(s)
        piece = 256
        shape = (2,) * (places - 1) + (rows, piece)
        for side in (1, 0):
            for column in range(0, CHUNK, piece):
                value = jnp.dot(
                    turned[side], grad[s, :, column : column + piece], preferred_element_type=WIDE
                ).astype(LOW)
                value = value.reshape(shape)
                at = (slice(None),) * (places - 1) + (slice(None), pl.ds(column, piece))
                if side:
                    sent[(s,) + at] = value
                else:
                    held[(t % slots,) + at] = value
        core_copy(t).start()

    for copy in loads(0, 0):
        copy.start()

    def iteration(t, carry):
        for k in reversed(range(plan.depth)):
            u = t - 2 - k

            @pl.when((u >= 0) & (u < chunks))
            def _():
                for i in range(len(plan.steps)):
                    if k < len(plan.steps[i]):
                        advance(i, k, u)

        u = t - 1

        @pl.when((u >= 0) & (u < chunks))
        def _():
            core_copy(u).wait()
            for i in range(len(plan.steps)):
                at = (slice(None),) * (places - 1) + (slice(None), pl.ds(*plan.columns[i]))
                here = (u % slots,) + at
                held[here] = held[here] + core_in[(u % 2,) + at]
                step_copy(i, 0, u).start()

        @pl.when(t < chunks)
        def _():
            make(t)

        return carry

    lax.fori_loop(0, chunks + plan.depth + 1, iteration, 0)


def reduced(pairs, frames, groups):
    count, inner = pairs[0][0].shape
    plan = Plan(frames, groups, inner)
    operands, sources = [], []
    for left, grad in pairs:
        at = len(operands)
        operands += [left, grad]
        sources += [(at, at + 1, column) for column in range(0, grad.shape[1], CHUNK)]
    chunks, slots = len(sources), plan.depth + 2
    half = (2,) * (plan.places - 1) + (plan.rows, CHUNK)
    steps = [step for steps in plan.steps for step in steps]
    scratch = [
        pltpu.VMEM((2, count, inner), LOW),
        pltpu.VMEM((2, count, CHUNK), LOW),
        pltpu.VMEM((2, inner // 2, count), LOW),
        pltpu.VMEM((2,) + half, LOW),
        pltpu.VMEM((slots,) + half, LOW),
        pltpu.VMEM((2,) + half, LOW),
        pltpu.SemaphoreType.DMA((2, 2)),
        pltpu.SemaphoreType.DMA((2,)),
        pltpu.SemaphoreType.DMA((2,)),
        pltpu.SemaphoreType.DMA((len(steps), 2)),
        pltpu.SemaphoreType.DMA((len(steps), 2)),
    ] + [pltpu.VMEM((2,) + step[-1], LOW) for step in steps]
    result = pl.pallas_call(
        partial(reduce_kernel, plan, sources, slots, len(operands)),
        out_shape=jax.ShapeDtypeStruct((chunks, plan.rows, CHUNK), WIDE),
        in_specs=[pl.BlockSpec(memory_space=pl.ANY)] * len(operands),
        out_specs=pl.BlockSpec(memory_space=pltpu.VMEM),
        scratch_shapes=scratch,
        compiler_params=pltpu.CompilerParams(
            collective_id=0, has_side_effects=True, vmem_limit_bytes=48 * MIB
        ),
        cost_estimate=pl.CostEstimate(
            flops=2 * count * inner * CHUNK * chunks * 5,
            bytes_accessed=4 * count * CHUNK * chunks,
            transcendentals=0,
        ),
        name="reduce",
    )(*operands)
    outs, at = [], 0
    for _, grad in pairs:
        parts = grad.shape[1] // CHUNK
        outs.append(jnp.concatenate([result[at + i] for i in range(parts)], axis=1))
        at += parts
    return outs


def body(
    parents,
    children,
    child_counts,
    out_grad,
    child_gain,
    cross_gain,
    cross_query,
    cross_keyval,
    cross_output,
    self_gain,
    self_project,
    self_output,
    mlp_gain,
    mlp_up,
    mlp_down,
):
    clips, half_rows, features = parents.shape
    nodes = clips // 2
    frames, groups = lax.axis_size("frames"), lax.axis_size("groups")
    frame = lax.axis_index("frames")
    other = flipped(frame, LEVEL)
    side = bit_of(frame, LEVEL)
    child_own, child_got = to_nodes(children)
    parent_own, parent_got = to_nodes(parents)
    grad_own, grad_got = to_nodes(out_grad)
    mine = lax.dynamic_slice_in_dim(child_counts, side * nodes, nodes, 0)
    counts = jnp.stack(
        [
            lax.dynamic_slice_in_dim(mine, frame, 1, 1)[:, 0],
            lax.dynamic_slice_in_dim(mine, other, 1, 1)[:, 0],
        ]
    )

    def flat(value):
        return value.reshape(-1, value.shape[-1])

    def rows4(value):
        return value.reshape(2, nodes, half_rows, value.shape[-1])

    def join(own, got):
        return flat(jnp.concatenate([own, got], axis=0))

    gain_child = child_gain.astype(WIDE)
    gain_cross = cross_gain.astype(WIDE)
    gain_self = self_gain.astype(WIDE)
    gain_mlp = mlp_gain.astype(WIDE)

    child_latents = join(child_own, child_got).astype(WIDE)
    latents = join(parent_own, parent_got).astype(WIDE)
    grad_low = join(grad_own, grad_got)

    child_in = layer_norm(child_latents, gain_child).astype(LOW)
    keyval = matmul(child_in, cross_keyval).astype(LOW)
    cross_in = layer_norm(latents, gain_cross).astype(LOW)
    queries = matmul(cross_in, cross_query).astype(LOW)
    cross_mixed = flat(attend(counts, rows4(queries), rows4(keyval), 0, True))
    after_cross = latents + matmul(cross_mixed, cross_output)
    self_in = layer_norm(after_cross, gain_self).astype(LOW)
    projected = matmul(self_in, self_project).astype(LOW)
    self_mixed = flat(attend(counts, rows4(projected), rows4(projected), 1, False))
    after_self = after_cross + matmul(self_mixed, self_output)
    mlp_in = layer_norm(after_self, gain_mlp).astype(LOW)
    activated, grad_hidden, fed, grad_mlp_in = feed(mlp_in, grad_low, mlp_up, mlp_down)
    top = (after_self + fed).astype(LOW).reshape(2, nodes, half_rows, features)
    top_latents = from_nodes(top[0], swapped(top[1], "frames", LEVEL))

    grad_down = weight_grad(activated, grad_low).astype(LOW)
    share_down = lax.psum_scatter(grad_down, "frames", scatter_dimension=0, tiled=True)

    grad_norm, gain_grad_mlp = norm_back(after_self, gain_mlp, grad_mlp_in)
    grad_after_self = grad_low.astype(WIDE) + grad_norm
    grad_self_out = grad_after_self.astype(LOW)
    grad_self_mix = product_back(grad_self_out, self_output).astype(LOW)
    (grad_projected,) = attend_back(
        counts, rows4(projected), rows4(projected), 1, False, rows4(grad_self_mix)
    )
    grad_projected = flat(grad_projected)
    grad_norm, gain_grad_self = norm_back(
        after_cross, gain_self, product_back(grad_projected, self_project)
    )
    grad_after_cross = grad_after_self + grad_norm
    grad_cross_out = grad_after_cross.astype(LOW)
    grad_cross_mix = product_back(grad_cross_out, cross_output).astype(LOW)
    grad_queries, grad_keyval = attend_back(
        counts, rows4(queries), rows4(keyval), 0, True, rows4(grad_cross_mix)
    )
    grad_queries, grad_keyval = flat(grad_queries), flat(grad_keyval)
    grad_norm, gain_grad_cross = norm_back(
        latents, gain_cross, product_back(grad_queries, cross_query)
    )
    grad_parents = rows4(grad_after_cross + grad_norm)
    grad_norm, gain_grad_child = norm_back(
        child_latents, gain_child, product_back(grad_keyval, cross_keyval)
    )
    grad_children = rows4(grad_norm)
    parents_back = swapped(grad_parents[1].astype(LOW), "frames", LEVEL).astype(WIDE)
    children_back = swapped(grad_children[1].astype(LOW), "frames", LEVEL).astype(WIDE)

    total_up, total_self_out, total_project, total_cross_out, total_query, total_keyval = reduced(
        [
            (mlp_in, grad_hidden),
            (self_mixed, grad_self_out),
            (self_in, grad_projected),
            (cross_mixed, grad_cross_out),
            (cross_in, grad_queries),
            (child_in, grad_keyval),
        ],
        frames,
        groups,
    )
    total_down = share_down
    for place in range(groups.bit_length() - 1):
        total_down = total_down + swapped(total_down, "groups", place)
    total_down = total_down.astype(WIDE)
    gains = jnp.stack([gain_grad_child, gain_grad_cross, gain_grad_self, gain_grad_mlp])
    gains = lax.psum(gains, ("frames", "groups"))
    width = features // frames
    gains = lax.dynamic_slice_in_dim(gains, frame * width, width, 1)
    return (
        top_latents,
        from_nodes(grad_parents[0], parents_back),
        from_nodes(grad_children[0], children_back),
        gains[0],
        gains[1],
        total_query,
        total_keyval,
        total_cross_out,
        gains[2],
        total_project,
        total_self_out,
        gains[3],
        total_up,
        total_down,
    )


def solution(mesh):
    rows = P("groups", "frames", None)
    shard, shard2 = P("frames"), P("frames", None)
    return jax.shard_map(
        body,
        mesh=mesh,
        in_specs=(rows, rows, P("groups", None), rows) + (P(),) * 11,
        out_specs=(
            rows,
            rows,
            rows,
            shard,
            shard,
            shard2,
            shard2,
            shard2,
            shard,
            shard2,
            shard2,
            shard,
            shard2,
            shard2,
        ),
        check_vma=False,
    )
```

```python
from functools import partial

import jax
import jax.numpy as jnp
from jax import lax
from jax.experimental import pallas as pl
from jax.experimental.pallas import tpu as pltpu
from jax.sharding import PartitionSpec as P

HEADS = 8
HEAD_DIM = 128
LEVEL = 1
SCALE = HEAD_DIM ** (-0.5)
LOW = jnp.bfloat16
WIDE = jnp.float32
MIB = 1 << 20


def bit_of(value, place):
    return (value // (1 << place)) % 2


def flipped(value, place):
    return value + (1 << place) - (2 << place) * bit_of(value, place)


def xor_static(constant, value, places):
    total = 0
    for place in range(places):
        bit = bit_of(value, place)
        total = total + ((1 - bit) if (constant >> place) & 1 else bit) * (1 << place)
    return total


def swapped(value, axis, place):
    mask = 1 << place
    return lax.ppermute(value, axis, [(s, s ^ mask) for s in range(lax.axis_size(axis))])


def to_nodes(value):
    half = value.shape[0] // 2
    side = bit_of(lax.axis_index("frames"), LEVEL)
    kept = lax.dynamic_slice_in_dim(value, side * half, half, 0)
    sent = lax.dynamic_slice_in_dim(value, (1 - side) * half, half, 0)
    return kept, swapped(sent, "frames", LEVEL)


def from_nodes(own, back):
    side = bit_of(lax.axis_index("frames"), LEVEL)
    first = jnp.concatenate([own, back], axis=0)
    second = jnp.concatenate([back, own], axis=0)
    return jnp.where(side == 0, first, second)


def layer_norm(values, gain):
    average = jnp.mean(values, axis=-1, keepdims=True)
    centred = values - average
    spread = jnp.mean(centred * centred, axis=-1, keepdims=True)
    return centred * lax.rsqrt(spread + 1e-05) * gain


def norm_back(values, gain, grad_out):
    average = jnp.mean(values, axis=-1, keepdims=True)
    centred = values - average
    spread = jnp.mean(centred * centred, axis=-1, keepdims=True)
    inverse = lax.rsqrt(spread + 1e-05)
    normed = centred * inverse
    scaled = grad_out * gain
    grad = inverse * (
        scaled
        - jnp.mean(scaled, axis=-1, keepdims=True)
        - normed * jnp.mean(scaled * normed, axis=-1, keepdims=True)
    )
    return grad, jnp.sum(grad_out * normed, axis=0)


def matmul(left, right):
    return jnp.dot(left, right, preferred_element_type=WIDE)


def product_back(grad_rows, weight):
    return lax.dot_general(
        grad_rows, weight, (((1,), (1,)), ((), ())), preferred_element_type=WIDE
    )


def weight_grad(inputs, grad_rows):
    return lax.dot_general(
        inputs, grad_rows, (((0,), (0,)), ((), ())), preferred_element_type=WIDE
    )


def dot_nt(left, right):
    return lax.dot_general(left, right, (((1,), (1,)), ((), ())), preferred_element_type=WIDE)


def dot_tn(left, right):
    return lax.dot_general(left, right, (((0,), (0,)), ((), ())), preferred_element_type=WIDE)


def node_rows(ref, head):
    block = ref[:, 0, :, head * HEAD_DIM : (head + 1) * HEAD_DIM]
    return block.reshape(block.shape[0] * block.shape[1], HEAD_DIM)


def valid_keys(count_ref, rows, shape, axis):
    node = pl.program_id(0)
    key = lax.broadcasted_iota(jnp.int32, shape, axis)
    first, second = count_ref[0, node], count_ref[1, node]
    return key < jnp.where(key < rows, first, second + rows)


def attend_kernel(masked, count_ref, q_ref, k_ref, v_ref, out_ref):
    heads = q_ref.shape[3] // HEAD_DIM
    rows = q_ref.shape[2]
    for head in range(heads):
        q, k, v = (node_rows(ref, head) for ref in (q_ref, k_ref, v_ref))
        scores = dot_nt(q, k) * SCALE
        if masked:
            scores = jnp.where(valid_keys(count_ref, rows, scores.shape, 1), scores, -1e30)
        top = jnp.max(scores, axis=1, keepdims=True)
        raised = jnp.exp(scores - top)
        weights = raised / jnp.sum(raised, axis=1, keepdims=True)
        mixed = jnp.dot(weights.astype(LOW), v, preferred_element_type=WIDE)
        out_ref[:, 0, :, head * HEAD_DIM : (head + 1) * HEAD_DIM] = mixed.astype(LOW).reshape(
            2, rows, HEAD_DIM
        )


def attend_back_kernel(masked, count_ref, q_ref, k_ref, v_ref, grad_ref, *outs):
    heads = q_ref.shape[3] // HEAD_DIM
    rows = q_ref.shape[2]
    wide = heads * HEAD_DIM
    places = [(outs[0], 0), (outs[-1], wide if len(outs) == 1 else 0)]
    places.append((outs[-1], places[1][1] + wide))
    for head in range(heads):
        q, k, v, grad = (node_rows(ref, head) for ref in (q_ref, k_ref, v_ref, grad_ref))
        scores = dot_nt(k, q) * SCALE
        if masked:
            scores = jnp.where(valid_keys(count_ref, rows, scores.shape, 0), scores, -1e30)
        top = jnp.max(scores, axis=0, keepdims=True)
        raised = jnp.exp(scores - top)
        weights = raised / jnp.sum(raised, axis=0, keepdims=True)
        grad_weights = dot_nt(v, grad)
        inner = jnp.sum(weights * grad_weights, axis=0, keepdims=True)
        grad_scores = (weights * (grad_weights - inner)).astype(LOW)
        results = (
            dot_tn(grad_scores, k) * SCALE,
            jnp.dot(grad_scores, q, preferred_element_type=WIDE) * SCALE,
            jnp.dot(weights.astype(LOW), grad, preferred_element_type=WIDE),
        )
        for (ref, start), result in zip(places, results):
            start = start + head * HEAD_DIM
            ref[:, 0, :, start : start + HEAD_DIM] = result.astype(LOW).reshape(2, rows, HEAD_DIM)


def column_block(rows, width, column):
    return pl.BlockSpec((2, 1, rows, width), lambda node, *_: (0, node, 0, column))


def attend(counts, queries, keyval, key_column, masked):
    _, nodes, rows, _ = queries.shape
    features = HEADS * HEAD_DIM
    spec = pltpu.PrefetchScalarGridSpec(
        num_scalar_prefetch=1,
        grid=(nodes,),
        in_specs=[column_block(rows, features, c) for c in (0, key_column, key_column + 1)],
        out_specs=column_block(rows, features, 0),
    )
    flops = 4 * nodes * HEADS * (2 * rows) ** 2 * HEAD_DIM
    return pl.pallas_call(
        partial(attend_kernel, masked),
        grid_spec=spec,
        out_shape=jax.ShapeDtypeStruct((2, nodes, rows, features), LOW),
        cost_estimate=pl.CostEstimate(
            flops=flops, bytes_accessed=8 * 2 * nodes * rows * features, transcendentals=flops // 512
        ),
        name="attend",
    )(counts, queries, keyval, keyval)


def attend_back(counts, queries, keyval, key_column, masked, grad_mix):
    _, nodes, rows, _ = queries.shape
    features = HEADS * HEAD_DIM
    widths = (3 * features,) if key_column == 1 else (features, 2 * features)
    spec = pltpu.PrefetchScalarGridSpec(
        num_scalar_prefetch=1,
        grid=(nodes,),
        in_specs=[column_block(rows, features, c) for c in (0, key_column, key_column + 1, 0)],
        out_specs=[column_block(rows, width, 0) for width in widths],
    )
    flops = 10 * nodes * HEADS * (2 * rows) ** 2 * HEAD_DIM
    return pl.pallas_call(
        partial(attend_back_kernel, masked),
        grid_spec=spec,
        out_shape=[jax.ShapeDtypeStruct((2, nodes, rows, width), LOW) for width in widths],
        cost_estimate=pl.CostEstimate(
            flops=flops, bytes_accessed=14 * 2 * nodes * rows * features, transcendentals=flops // 1280
        ),
        name="attend_back",
    )(counts, queries, keyval, keyval, grad_mix)


def feed_kernel(in_ref, grad_ref, up_ref, down_ref, act_ref, grad_hidden_ref, out_ref, grad_in_ref):
    step = pl.program_id(0)

    @pl.when(step == 0)
    def _():
        out_ref[...] = jnp.zeros_like(out_ref)
        grad_in_ref[...] = jnp.zeros_like(grad_in_ref)

    rows = in_ref.shape[0]
    part = rows // 2
    for start in range(0, rows, part):
        here = pl.ds(start, part)
        hidden = jnp.dot(in_ref[here, :], up_ref[...], preferred_element_type=WIDE)
        grad_act = dot_nt(grad_ref[here, :], down_ref[...])
        normal = 0.5 * (1.0 + lax.erf(hidden * 0.7071067811865476))
        density = jnp.exp(-0.5 * hidden * hidden) * 0.3989422804014327
        act = (hidden * normal).astype(LOW)
        grad_hidden = (grad_act * (normal + hidden * density)).astype(LOW)
        act_ref[here, :] = act
        grad_hidden_ref[here, :] = grad_hidden
        out_ref[here, :] += jnp.dot(act, down_ref[...], preferred_element_type=WIDE)
        grad_in_ref[here, :] += dot_nt(grad_hidden, up_ref[...])


def feed(mlp_in, grad_low, mlp_up, mlp_down):
    rows, features = mlp_in.shape
    hidden = mlp_up.shape[1]
    tile = min(512, hidden)
    whole = pl.BlockSpec((rows, features), lambda i: (0, 0))
    return pl.pallas_call(
        feed_kernel,
        grid=(hidden // tile,),
        in_specs=[
            whole,
            whole,
            pl.BlockSpec((features, tile), lambda i: (0, i)),
            pl.BlockSpec((tile, features), lambda i: (i, 0)),
        ],
        out_specs=[
            pl.BlockSpec((rows, tile), lambda i: (0, i)),
            pl.BlockSpec((rows, tile), lambda i: (0, i)),
            whole,
            whole,
        ],
        out_shape=[
            jax.ShapeDtypeStruct((rows, hidden), LOW),
            jax.ShapeDtypeStruct((rows, hidden), LOW),
            jax.ShapeDtypeStruct((rows, features), WIDE),
            jax.ShapeDtypeStruct((rows, features), WIDE),
        ],
        compiler_params=pltpu.CompilerParams(vmem_limit_bytes=40 * MIB),
        cost_estimate=pl.CostEstimate(
            flops=8 * rows * features * hidden,
            bytes_accessed=4 * features * hidden + 12 * rows * hidden,
            transcendentals=2 * rows * hidden,
        ),
        name="feed",
    )(mlp_in, grad_low, mlp_up, mlp_down)


CHUNK = 1024
SHARES = (512, 256, 256)


class Plan:
    def __init__(self, frames, groups, inner):
        self.frames, self.groups = frames, groups
        self.places = frames.bit_length() - 1
        self.group_places = groups.bit_length() - 1
        self.rows = inner // frames
        self.split = groups == 2 and self.rows % 32 == 0
        self.part = self.rows // 2 if self.split else self.rows
        near, far = [("f", 1)], [("f", d) for d in range(2, self.places)]
        if self.split:
            cut, join, add = [("cut", 0)], [("join", 0)], [("add", 0)]
            self.orders = [near + cut + far + join, cut + far + near + join, far + near + add]
        else:
            add = [("add", e) for e in range(self.group_places)]
            self.orders = [near + far + add, far + near + add, far + near + add]
        self.depth = max(len(order) for order in self.orders)
        starts = [0]
        for share in SHARES:
            starts.append(starts[-1] + share)
        self.columns = [(starts[i], SHARES[i]) for i in range(len(SHARES))]
        self.steps = []
        for (start, width), order in zip(self.columns, self.orders):
            fixed, size, steps = {}, self.rows, []
            for kind, place in order:
                free = [d for d in range(1, self.places) if d not in fixed]
                if kind == "f":
                    send, keep = dict(fixed), dict(fixed)
                    send[place], keep[place] = 1, 0
                    send_rows = keep_rows = (0, size)
                    fixed[place] = 0
                    free.remove(place)
                elif kind == "cut":
                    send = keep = dict(fixed)
                    send_rows, keep_rows = (self.part, self.part), (0, self.part)
                    size = self.part
                else:
                    send = keep = dict(fixed)
                    send_rows = keep_rows = (0, size)
                shape = (2,) * len(free) + (send_rows[1], width)
                steps.append((kind, place, send, send_rows, keep, keep_rows, shape))
            self.steps.append(steps)

    def index(self, slot, fixed, rows, columns):
        middle = [fixed.get(d, slice(None)) for d in reversed(range(1, self.places))]
        return tuple([slot] + middle + [pl.ds(*rows), pl.ds(*columns)])


def reduce_kernel(plan, sources, slots, n_in, *refs):
    ins, gain_ref, out_ref, gain_out, rest = refs[:n_in], refs[n_in], refs[n_in + 1], refs[n_in + 2], refs[n_in + 3 :]
    raw, grad, turned, sent, held, core_in, gain_sum, gain_land = rest[:8]
    load_sem, core_send, core_recv, send_sem, recv_sem, gain_send, gain_recv = rest[8:15]
    lands = rest[15:]
    inner = turned.shape[2] * 2
    chunks = len(sources)
    frame, group = lax.axis_index("frames"), lax.axis_index("groups")
    rows, part, places = plan.rows, plan.part, plan.places
    halves = rows // part
    blocks = plan.frames // 2

    ids, count = {}, 0
    for i, steps in enumerate(plan.steps):
        for k in range(len(steps)):
            ids[i, k] = count
            count += 1

    def partner(kind, place):
        if kind == "f":
            return {"frames": flipped(frame, place), "groups": group}
        return {"frames": frame, "groups": flipped(group, place)}

    barrier = pltpu.get_barrier_semaphore()
    everyone = [partner("f", d) for d in range(places)] + [
        partner("g", e) for e in range(plan.group_places)
    ]
    for device in everyone:
        pl.semaphore_signal(barrier, inc=1, device_id=device, device_id_type=pl.DeviceIdType.MESH)
    pl.semaphore_wait(barrier, len(everyone))

    def core_copy(u):
        s = u % 2
        return pltpu.make_async_remote_copy(
            src_ref=sent.at[s],
            dst_ref=core_in.at[s],
            send_sem=core_send.at[s],
            recv_sem=core_recv.at[s],
            device_id=partner("f", 0),
            device_id_type=pl.DeviceIdType.MESH,
        )

    def step_copy(i, k, u):
        kind, place, send, send_rows, _, _, _ = plan.steps[i][k]
        s = u % 2
        return pltpu.make_async_remote_copy(
            src_ref=held.at[plan.index(u % slots, send, send_rows, plan.columns[i])],
            dst_ref=lands[ids[i, k]].at[s],
            send_sem=send_sem.at[ids[i, k], s],
            recv_sem=recv_sem.at[ids[i, k], s],
            device_id=partner(kind, place),
            device_id_type=pl.DeviceIdType.MESH,
        )

    def grad_load(t, which):
        right, column = sources[which][1:3]
        return pltpu.make_async_copy(
            ins[right].at[:, column : column + CHUNK], grad.at[t % 2], load_sem.at[t % 2]
        )

    def left_start(which):
        left, group_of = sources[which][0], sources[which][3]
        if group_of is None:
            pltpu.make_async_copy(ins[left], raw.at[:, 0:inner], load_sem.at[2]).start()
            return
        per_block = ins[left].shape[1] // plan.frames // 128
        for block in range(plan.frames):
            pltpu.make_async_copy(
                ins[left].at[:, pl.ds((block * per_block + group_of) * 128, 128)],
                raw.at[:, pl.ds(block * 128, 128)],
                load_sem.at[3],
            ).start()

    def left_wait(which):
        left, group_of = sources[which][0], sources[which][3]
        width, place = (inner, 2) if group_of is None else (plan.frames * 128, 3)
        pltpu.make_async_copy(
            ins[left].at[:, 0:width], raw.at[:, 0:width], load_sem.at[place]
        ).wait()

    def start_loads(which, t):
        grad_load(t, which).start()
        if sources[which][5]:
            left_start(which)

    def row_place(half):
        if halves == 1:
            return 0
        place = bit_of(group, 0)
        return ((1 - place) if half else place) * part

    def finish(i, k, u):
        kind, _, _, _, keep, keep_rows, _ = plan.steps[i][k]
        start, width = plan.columns[i]
        land = lands[ids[i, k]]
        s = u % 2
        if kind == "join":
            mine = held[plan.index(u % slots, keep, (0, part), plan.columns[i])]
            other = land[s]
            for half, value in ((0, mine), (1, other)):
                at = pl.multiple_of(row_place(half), part)
                out_ref[u, pl.ds(at, part), pl.ds(start, width)] = value.astype(WIDE)
        else:
            for half in range(halves):
                source = (halves - 1 - half) * part
                mine = held[plan.index(u % slots, keep, (half * part, part), plan.columns[i])]
                other = land[s, pl.ds(source, part), :]
                at = pl.multiple_of(row_place(half), part)
                out_ref[u, pl.ds(at, part), pl.ds(start, width)] = mine.astype(WIDE) + other.astype(WIDE)

    def advance(i, k, u):
        step_copy(i, k, u).wait()
        if k == len(plan.steps[i]) - 1:
            finish(i, k, u)
            return
        _, _, _, _, keep, keep_rows, _ = plan.steps[i][k]
        at = plan.index(u % slots, keep, keep_rows, plan.columns[i])
        held[at] = held[at] + lands[ids[i, k]][u % 2]
        step_copy(i, k + 1, u).start()

    def turn_tile(value, at):
        for piece in range(128 // part):
            slot, block, half = at(piece)
            where = xor_static(block, frame, places)
            row = (where // 2) * rows
            if halves > 1:
                row = row + xor_static(half, group, 1) * part
            row = pl.multiple_of(row, part)
            turned[slot, where % 2, pl.ds(row, part), :] = value[piece * part : (piece + 1) * part, :]

    def turn(stacked):
        for tile in range(plan.frames if stacked else inner // 128):
            value = raw[:, tile * 128 : (tile + 1) * 128].T

            def at(piece, tile=tile):
                if stacked:
                    return piece // halves, tile, piece % halves
                run = tile * (128 // part) + piece
                return 0, run // halves, run % halves

            turn_tile(value, at)

    def any_of(t, choices):
        found = t == choices[0]
        for choice in choices[1:]:
            found = found | (t == choice)
        return found

    def make(t):
        s = t % 2
        grad_load(t, 0).wait()
        for stacked in (True, False):
            fresh = [w for w in range(chunks) if sources[w][5] and (sources[w][3] is not None) == stacked]
            if fresh:

                @pl.when(any_of(t, fresh))
                def _():
                    left_wait(fresh[0])
                    turn(stacked)

        for which in range(1, chunks):

            @pl.when(t + 1 == which)
            def _():
                start_loads(which, t + 1)

        tslot = 0
        for which in range(chunks):
            if sources[which][4]:
                tslot = jnp.where(t == which, sources[which][4], tslot)
        piece = 256
        shape = (2,) * (places - 1) + (rows, piece)
        for side in (1, 0):
            for column in range(0, CHUNK, piece):
                value = jnp.dot(
                    turned[tslot, side], grad[s, :, column : column + piece], preferred_element_type=WIDE
                ).astype(LOW)
                value = value.reshape(shape)
                at = (slice(None),) * (places - 1) + (slice(None), pl.ds(column, piece))
                if side:
                    sent[(s,) + at] = value
                else:
                    held[(t % slots,) + at] = value
        core_copy(t).start()

    gain_steps = [("f", d) for d in range(places)] + [("g", e) for e in range(plan.group_places)]

    def gain_copy(k):
        return pltpu.make_async_remote_copy(
            src_ref=gain_sum,
            dst_ref=gain_land.at[k],
            send_sem=gain_send.at[k],
            recv_sem=gain_recv.at[k],
            device_id=partner(*gain_steps[k]),
            device_id_type=pl.DeviceIdType.MESH,
        )

    def gain_work(t):
        @pl.when(t == 0)
        def _():
            gain_sum[...] = gain_ref[...]

        for k in range(len(gain_steps) + 1):

            @pl.when(t == k + 1)
            def _():
                if k:
                    gain_copy(k - 1).wait()
                    gain_sum[...] = gain_sum[...] + gain_land[k - 1]
                if k < len(gain_steps):
                    gain_copy(k).start()
                else:
                    gain_out[...] = gain_sum[...]

    start_loads(0, 0)

    def iteration(t, carry):
        for k in reversed(range(plan.depth)):
            u = t - 2 - k

            @pl.when((u >= 0) & (u < chunks))
            def _():
                for i in range(len(plan.steps)):
                    if k < len(plan.steps[i]):
                        advance(i, k, u)

        u = t - 1

        @pl.when((u >= 0) & (u < chunks))
        def _():
            core_copy(u).wait()
            for i in range(len(plan.steps)):
                at = (slice(None),) * (places - 1) + (slice(None), pl.ds(*plan.columns[i]))
                here = (u % slots,) + at
                held[here] = held[here] + core_in[(u % 2,) + at]
                step_copy(i, 0, u).start()

        @pl.when(t < chunks)
        def _():
            make(t)

        gain_work(t)
        return carry

    lax.fori_loop(0, chunks + plan.depth + 1, iteration, 0)


def reduced(pairs, gains, frames, groups):
    count = pairs[0][0].shape[0]
    inner = min(left.shape[1] for left, _ in pairs)
    plan = Plan(frames, groups, inner)
    per_tile = max(1, 128 // plan.rows)
    operands, sources = [], []
    for left, grad in pairs:
        at = len(operands)
        operands += [left, grad]
        stack = left.shape[1] // inner
        if stack > 1:
            for i in range(stack):
                sources.append((at, at + 1, 0, i // per_tile, i % per_tile, i % per_tile == 0))
        else:
            for column in range(0, grad.shape[1], CHUNK):
                sources.append((at, at + 1, column, None, 0, column == 0))
    chunks, slots = len(sources), plan.depth + 2
    half = (2,) * (plan.places - 1) + (plan.rows, CHUNK)
    steps = [step for steps in plan.steps for step in steps]
    gain_steps = plan.places + plan.group_places
    gain_shape = (gains.size // 128, 128)
    scratch = [
        pltpu.VMEM((count, frames * 128), LOW),
        pltpu.VMEM((2, count, CHUNK), LOW),
        pltpu.VMEM((per_tile, 2, inner // 2, count), LOW),
        pltpu.VMEM((2,) + half, LOW),
        pltpu.VMEM((slots,) + half, LOW),
        pltpu.VMEM((2,) + half, LOW),
        pltpu.VMEM(gain_shape, WIDE),
        pltpu.VMEM((gain_steps,) + gain_shape, WIDE),
        pltpu.SemaphoreType.DMA((4,)),
        pltpu.SemaphoreType.DMA((2,)),
        pltpu.SemaphoreType.DMA((2,)),
        pltpu.SemaphoreType.DMA((len(steps), 2)),
        pltpu.SemaphoreType.DMA((len(steps), 2)),
        pltpu.SemaphoreType.DMA((gain_steps,)),
        pltpu.SemaphoreType.DMA((gain_steps,)),
    ] + [pltpu.VMEM((2,) + step[-1], LOW) for step in steps]
    in_vmem = pl.BlockSpec(memory_space=pltpu.VMEM)
    result, gain_total = pl.pallas_call(
        partial(reduce_kernel, plan, sources, slots, len(operands)),
        out_shape=[
            jax.ShapeDtypeStruct((chunks, plan.rows, CHUNK), WIDE),
            jax.ShapeDtypeStruct(gain_shape, WIDE),
        ],
        in_specs=[pl.BlockSpec(memory_space=pl.ANY)] * len(operands) + [in_vmem],
        out_specs=[in_vmem, in_vmem],
        scratch_shapes=scratch,
        compiler_params=pltpu.CompilerParams(
            collective_id=0, has_side_effects=True, vmem_limit_bytes=48 * MIB
        ),
        cost_estimate=pl.CostEstimate(
            flops=2 * count * inner * CHUNK * chunks * 5,
            bytes_accessed=4 * count * CHUNK * chunks,
            transcendentals=0,
        ),
        name="reduce",
    )(*operands, gains.reshape(gain_shape))
    outs, at = [], 0
    for left, grad in pairs:
        stack, parts = left.shape[1] // inner, grad.shape[1] // CHUNK
        if stack > 1:
            outs.append(result[at : at + stack].reshape(stack * plan.rows, CHUNK))
            at += stack
        else:
            outs.append(jnp.concatenate([result[at + i] for i in range(parts)], axis=1))
            at += parts
    return outs, gain_total.reshape(gains.shape)


def body(
    parents,
    children,
    child_counts,
    out_grad,
    child_gain,
    cross_gain,
    cross_query,
    cross_keyval,
    cross_output,
    self_gain,
    self_project,
    self_output,
    mlp_gain,
    mlp_up,
    mlp_down,
):
    clips, half_rows, features = parents.shape
    nodes = clips // 2
    frames, groups = lax.axis_size("frames"), lax.axis_size("groups")
    frame = lax.axis_index("frames")
    other = flipped(frame, LEVEL)
    side = bit_of(frame, LEVEL)
    child_own, child_got = to_nodes(children)
    parent_own, parent_got = to_nodes(parents)
    grad_own, grad_got = to_nodes(out_grad)
    mine = lax.dynamic_slice_in_dim(child_counts, side * nodes, nodes, 0)
    counts = jnp.stack(
        [
            lax.dynamic_slice_in_dim(mine, frame, 1, 1)[:, 0],
            lax.dynamic_slice_in_dim(mine, other, 1, 1)[:, 0],
        ]
    )

    def flat(value):
        return value.reshape(-1, value.shape[-1])

    def rows4(value):
        return value.reshape(2, nodes, half_rows, value.shape[-1])

    def join(own, got):
        return flat(jnp.concatenate([own, got], axis=0))

    gain_child = child_gain.astype(WIDE)
    gain_cross = cross_gain.astype(WIDE)
    gain_self = self_gain.astype(WIDE)
    gain_mlp = mlp_gain.astype(WIDE)

    child_latents = join(child_own, child_got).astype(WIDE)
    latents = join(parent_own, parent_got).astype(WIDE)
    grad_low = join(grad_own, grad_got)

    child_in = layer_norm(child_latents, gain_child).astype(LOW)
    keyval = matmul(child_in, cross_keyval).astype(LOW)
    cross_in = layer_norm(latents, gain_cross).astype(LOW)
    queries = matmul(cross_in, cross_query).astype(LOW)
    cross_mixed = flat(attend(counts, rows4(queries), rows4(keyval), 0, True))
    after_cross = latents + matmul(cross_mixed, cross_output)
    self_in = layer_norm(after_cross, gain_self).astype(LOW)
    projected = matmul(self_in, self_project).astype(LOW)
    self_mixed = flat(attend(counts, rows4(projected), rows4(projected), 1, False))
    after_self = after_cross + matmul(self_mixed, self_output)
    mlp_in = layer_norm(after_self, gain_mlp).astype(LOW)
    activated, grad_hidden, fed, grad_mlp_in = feed(mlp_in, grad_low, mlp_up, mlp_down)
    top = (after_self + fed).astype(LOW).reshape(2, nodes, half_rows, features)
    top_latents = from_nodes(top[0], swapped(top[1], "frames", LEVEL))

    grad_norm, gain_grad_mlp = norm_back(after_self, gain_mlp, grad_mlp_in)
    grad_after_self = grad_low.astype(WIDE) + grad_norm
    grad_self_out = grad_after_self.astype(LOW)
    grad_self_mix = product_back(grad_self_out, self_output).astype(LOW)
    (grad_projected,) = attend_back(
        counts, rows4(projected), rows4(projected), 1, False, rows4(grad_self_mix)
    )
    grad_projected = flat(grad_projected)
    grad_norm, gain_grad_self = norm_back(
        after_cross, gain_self, product_back(grad_projected, self_project)
    )
    grad_after_cross = grad_after_self + grad_norm
    grad_cross_out = grad_after_cross.astype(LOW)
    grad_cross_mix = product_back(grad_cross_out, cross_output).astype(LOW)
    grad_queries, grad_keyval = attend_back(
        counts, rows4(queries), rows4(keyval), 0, True, rows4(grad_cross_mix)
    )
    grad_queries, grad_keyval = flat(grad_queries), flat(grad_keyval)
    grad_norm, gain_grad_cross = norm_back(
        latents, gain_cross, product_back(grad_queries, cross_query)
    )
    grad_parents = rows4(grad_after_cross + grad_norm)
    grad_norm, gain_grad_child = norm_back(
        child_latents, gain_child, product_back(grad_keyval, cross_keyval)
    )
    grad_children = rows4(grad_norm)
    parents_back = swapped(grad_parents[1].astype(LOW), "frames", LEVEL).astype(WIDE)
    children_back = swapped(grad_children[1].astype(LOW), "frames", LEVEL).astype(WIDE)

    gains = jnp.stack([gain_grad_child, gain_grad_cross, gain_grad_self, gain_grad_mlp])
    totals, gains = reduced(
        [
            (activated, grad_low),
            (mlp_in, grad_hidden),
            (self_mixed, grad_self_out),
            (self_in, grad_projected),
            (cross_mixed, grad_cross_out),
            (cross_in, grad_queries),
            (child_in, grad_keyval),
        ],
        gains,
        frames,
        groups,
    )
    total_down, total_up, total_self_out, total_project, total_cross_out, total_query, total_keyval = totals
    width = features // frames
    gains = lax.dynamic_slice_in_dim(gains, frame * width, width, 1)
    return (
        top_latents,
        from_nodes(grad_parents[0], parents_back),
        from_nodes(grad_children[0], children_back),
        gains[0],
        gains[1],
        total_query,
        total_keyval,
        total_cross_out,
        gains[2],
        total_project,
        total_self_out,
        gains[3],
        total_up,
        total_down,
    )


def solution(mesh):
    rows = P("groups", "frames", None)
    shard, shard2 = P("frames"), P("frames", None)
    return jax.shard_map(
        body,
        mesh=mesh,
        in_specs=(rows, rows, P("groups", None), rows) + (P(),) * 11,
        out_specs=(
            rows,
            rows,
            rows,
            shard,
            shard,
            shard2,
            shard2,
            shard2,
            shard,
            shard2,
            shard2,
            shard,
            shard2,
            shard2,
        ),
        check_vma=False,
    )
```

```python
from functools import partial

import jax
import jax.numpy as jnp
from jax import lax
from jax.experimental import pallas as pl
from jax.experimental.pallas import tpu as pltpu
from jax.sharding import PartitionSpec as P

HEADS = 8
HEAD_DIM = 128
LEVEL = 1
SCALE = HEAD_DIM ** (-0.5)
LOW = jnp.bfloat16
WIDE = jnp.float32
MIB = 1 << 20


def bit_of(value, place):
    return (value // (1 << place)) % 2


def flipped(value, place):
    return value + (1 << place) - (2 << place) * bit_of(value, place)


def xor_static(constant, value, places):
    total = 0
    for place in range(places):
        bit = bit_of(value, place)
        total = total + ((1 - bit) if (constant >> place) & 1 else bit) * (1 << place)
    return total


def dot_nt(left, right):
    return lax.dot_general(left, right, (((1,), (1,)), ((), ())), preferred_element_type=WIDE)


def dot_tn(left, right):
    return lax.dot_general(left, right, (((0,), (0,)), ((), ())), preferred_element_type=WIDE)


class Names:
    def __init__(self, names, refs):
        for name, ref in zip(names, refs, strict=True):
            setattr(self, name, ref)


GAINS = list(
    dict(
        child_gain=0, cross_gain=0, self_gain=0, mlp_gain=0,
    )
)
FORWARD_IN = list(
    dict(
        parents=0, children=0, out_grad=0, cross_query=0,
        cross_keyval=0, cross_output=0, self_project=0, self_output=0,
    )
)
FORWARD_OUT = list(
    dict(
        child_low=0, parent_low=0, grad_low=0, child_in=0,
        cross_in=0, keyval=0, queries=0, cross_mixed=0,
        after_cross=0, self_in=0, projected=0, self_mixed=0,
        after_self=0, mlp_in=0,
    )
)


def forward_kernel(*refs):
    names = ["counts"] + GAINS + FORWARD_IN + ["to_" + name for name in FORWARD_OUT] + FORWARD_OUT
    names += list(
        dict(
            w_query=0, w_keyval=0, w_output=0, w_project=0,
            w_self_output=0, load_sem=0, store_sem=0, send_sem=0,
            recv_sem=0,
        )
    )
    r = Names(names, refs)
    frame, group = lax.axis_index("frames"), lax.axis_index("groups")
    side = bit_of(frame, LEVEL)
    partner = {"frames": flipped(frame, LEVEL), "groups": group}
    nodes, rows_each, features = r.parents.shape[0] // 2, r.parents.shape[1], r.parents.shape[2]
    half_count = nodes * rows_each

    def rows(half):
        return pl.ds(half * half_count, half_count)

    own = []
    for i, (source, target) in enumerate(
        ((r.children, r.child_low), (r.parents, r.parent_low), (r.out_grad, r.grad_low))
    ):
        for node in range(nodes):
            own.append(
                pltpu.make_async_copy(
                    source.at[side * nodes + node],
                    target.at[pl.ds(node * rows_each, rows_each), :],
                    r.load_sem.at[i * nodes + node],
                )
            )
    for copy in own[: 2 * nodes]:
        copy.start()
    weights = {}
    held = dict(
        cross_keyval=r.w_keyval,
        cross_query=r.w_query,
        cross_output=r.w_output,
        self_project=r.w_project,
        self_output=r.w_self_output,
    )
    for i, (name, target) in enumerate(held.items()):
        weights[name] = pltpu.make_async_copy(getattr(r, name), target, r.load_sem.at[3 * nodes + i])
        weights[name].start()
    for copy in own[2 * nodes :]:
        copy.start()

    barrier = pltpu.get_barrier_semaphore()
    pl.semaphore_signal(barrier, inc=1, device_id=partner, device_id_type=pl.DeviceIdType.MESH)
    pl.semaphore_wait(barrier, 1)

    def swap(i, source, target):
        return [
            pltpu.make_async_remote_copy(
                src_ref=source.at[(1 - side) * nodes + node],
                dst_ref=target.at[pl.ds(half_count + node * rows_each, rows_each), :],
                send_sem=r.send_sem.at[i, node],
                recv_sem=r.recv_sem.at[i, node],
                device_id=partner,
                device_id_type=pl.DeviceIdType.MESH,
            )
            for node in range(nodes)
        ]

    swaps = [
        swap(0, r.children, r.child_low),
        swap(1, r.parents, r.parent_low),
        swap(2, r.out_grad, r.grad_low),
    ]
    for copies in swaps:
        for copy in copies:
            copy.start()

    stores = []

    def store(*which):
        for name in which:
            copy = pltpu.make_async_copy(
                getattr(r, name), getattr(r, "to_" + name), r.store_sem.at[FORWARD_OUT.index(name)]
            )
            copy.start()
            stores.append(copy)

    def norm(source, target, gain_at, half):
        gain = getattr(r, GAINS[gain_at])[...].astype(WIDE).reshape(1, features)
        step = 32

        def piece(i, carry):
            at = pl.ds(pl.multiple_of(half * half_count + i * step, step), step)
            values = source[at, :].astype(WIDE)
            average = jnp.mean(values, axis=-1, keepdims=True)
            centred = values - average
            spread = jnp.mean(centred * centred, axis=-1, keepdims=True)
            target[at, :] = (centred * lax.rsqrt(spread + 1e-05) * gain).astype(LOW)
            return carry

        lax.fori_loop(0, half_count // step, piece, 0, unroll=2)

    def product(source, weight, target, half, base=None):
        left = source[rows(half), :]
        for column in range(0, weight.shape[1], 256):
            here = slice(column, column + 256)
            value = jnp.dot(left, weight[:, here], preferred_element_type=WIDE)
            if base is not None:
                value = value + base[rows(half), here].astype(WIDE)
            target[rows(half), here] = value.astype(target.dtype)

    def attend(q_ref, kv_ref, k_at, v_at, target, halves, masked):
        for node in range(nodes):
            own_rows = slice(node * rows_each, (node + 1) * rows_each)
            got_rows = slice(half_count + node * rows_each, half_count + (node + 1) * rows_each)
            places = [(own_rows, got_rows)[half] for half in halves]
            for head in range(HEADS):

                def both(ref, at, which):
                    here = slice(at + head * HEAD_DIM, at + (head + 1) * HEAD_DIM)
                    parts = [ref[place, here] for place in which]
                    return parts[0] if len(parts) == 1 else jnp.concatenate(parts, axis=0)

                q = both(q_ref, 0, places)
                k, v = both(kv_ref, k_at, (own_rows, got_rows)), both(kv_ref, v_at, (own_rows, got_rows))
                scores = dot_nt(q, k) * SCALE
                if masked:
                    key = lax.broadcasted_iota(jnp.int32, scores.shape, 1)
                    clip = side * nodes + node
                    far = r.counts[clip, flipped(frame, LEVEL)] + rows_each
                    limit = jnp.where(key < rows_each, r.counts[clip, frame], far)
                    scores = jnp.where(key < limit, scores, -1e30)
                top = jnp.max(scores, axis=1, keepdims=True)
                raised = jnp.exp(scores - top)
                weight = raised / jnp.sum(raised, axis=1, keepdims=True)
                mixed = jnp.dot(weight.astype(LOW), v, preferred_element_type=WIDE).astype(LOW)
                for i, place in enumerate(places):
                    target[place, head * HEAD_DIM : (head + 1) * HEAD_DIM] = mixed[
                        i * rows_each : (i + 1) * rows_each
                    ]

    for copy in own[: 2 * nodes]:
        copy.wait()
    norm(r.child_low, r.child_in, 0, 0)
    weights["cross_keyval"].wait()
    product(r.child_in, r.w_keyval, r.keyval, 0)
    norm(r.parent_low, r.cross_in, 1, 0)
    weights["cross_query"].wait()
    product(r.cross_in, r.w_query, r.queries, 0)
    for copy in swaps[0]:
        copy.wait()
    norm(r.child_low, r.child_in, 0, 1)
    product(r.child_in, r.w_keyval, r.keyval, 1)
    store("child_low", "child_in", "keyval")
    weights["cross_output"].wait()
    weights["self_project"].wait()

    def rest_of_cross(half):
        attend(r.queries, r.keyval, 0, features, r.cross_mixed, (half,), True)
        product(r.cross_mixed, r.w_output, r.after_cross, half, r.parent_low)
        norm(r.after_cross, r.self_in, 2, half)
        product(r.self_in, r.w_project, r.projected, half)

    rest_of_cross(0)
    for copy in swaps[1]:
        copy.wait()
    norm(r.parent_low, r.cross_in, 1, 1)
    product(r.cross_in, r.w_query, r.queries, 1)
    store("parent_low", "cross_in", "queries")
    rest_of_cross(1)
    store("cross_mixed", "after_cross", "self_in", "projected")

    attend(r.projected, r.projected, features, 2 * features, r.self_mixed, (0, 1), False)
    store("self_mixed")
    weights["self_output"].wait()
    for half in (0, 1):
        product(r.self_mixed, r.w_self_output, r.after_self, half, r.after_cross)
        norm(r.after_self, r.mlp_in, 3, half)
    store("after_self", "mlp_in")
    for copy in own[2 * nodes :]:
        copy.wait()
    for copy in swaps[2]:
        copy.wait()
    store("grad_low")
    for copy in stores:
        copy.wait()


def forward(counts, values):
    clips, rows_each, features = values["parents"].shape
    nodes, count = clips // 2, clips * rows_each
    wide = {"keyval": 2, "projected": 3}
    shapes = {
        name: jax.ShapeDtypeStruct(
            (count, wide.get(name, 1) * features), WIDE if name.startswith("after") else LOW
        )
        for name in FORWARD_OUT
    }
    vmem, dma = pltpu.VMEM, pltpu.SemaphoreType.DMA
    results = pl.pallas_call(
        forward_kernel,
        out_shape=[shapes[name] for name in FORWARD_OUT],
        in_specs=[pl.BlockSpec(memory_space=pltpu.SMEM)]
        + [pl.BlockSpec(memory_space=vmem)] * len(GAINS)
        + [pl.BlockSpec(memory_space=pl.ANY)] * len(FORWARD_IN),
        out_specs=[pl.BlockSpec(memory_space=pl.ANY)] * len(FORWARD_OUT),
        scratch_shapes=[vmem(shapes[name].shape, shapes[name].dtype) for name in FORWARD_OUT]
        + [
            vmem((features, k * features), LOW) for k in (1, 2, 1, 3, 1)
        ]
        + [
            dma((3 * nodes + 5,)),
            dma((len(FORWARD_OUT),)),
            dma((3, nodes)),
            dma((3, nodes)),
        ],
        compiler_params=pltpu.CompilerParams(
            collective_id=1, has_side_effects=True, vmem_limit_bytes=56 * MIB
        ),
        cost_estimate=pl.CostEstimate(
            flops=18 * count * features * features, bytes_accessed=40 * count * features, transcendentals=0
        ),
        name="forward",
    )(counts, *[values[name] for name in GAINS + FORWARD_IN])
    return dict(zip(FORWARD_OUT, results))


CHUNK = 1024
SHARES = (384, 512, 128)
FEED = 512


class Plan:
    def __init__(self, frames, groups, inner):
        self.frames, self.groups = frames, groups
        self.places = frames.bit_length() - 1
        self.group_places = groups.bit_length() - 1
        self.rows = inner // frames
        self.split = groups == 2 and self.rows % 32 == 0
        self.part = self.rows // 2 if self.split else self.rows
        near, far = [("f", 1)], [("f", d) for d in range(2, self.places)]
        if self.split:
            cut, join, add = [("cut", 0)], [("join", 0)], [("add", 0)]
            self.orders = [near + cut + far + join, cut + far + near + join, far + near + add]
        else:
            add = [("add", e) for e in range(self.group_places)]
            self.orders = [near + far + add, far + near + add, far + near + add]
        self.depth = max(len(order) for order in self.orders)
        self.lag = 2 if self.depth <= 5 else 1
        self.lands = 2 * self.lag
        starts = [0]
        for share in SHARES:
            starts.append(starts[-1] + share)
        self.columns = [(starts[i], SHARES[i]) for i in range(len(SHARES))]
        self.axes, self.tiles, self.steps = [], [], []
        for (_, width), order in zip(self.columns, self.orders):
            axes = [step for step in order if step[0] in ("f", "cut")]
            size = self.part if ("cut", 0) in axes else self.rows
            self.axes.append(axes)
            self.tiles.append((2,) * len(axes) + (size, width))
            steps = []
            for number, (kind, place) in enumerate(order):
                if number < len(axes):
                    send, keep = (0,) * number + (1,), (0,) * (number + 1)
                else:
                    send = keep = (0,) * len(axes)
                shape = (2,) * (len(axes) - len(send)) + (size, width)
                steps.append((kind, place, send, keep, shape))
            self.steps.append(steps)


def attend_back_head(limits, rows, q, k, v, grad):
    scores = dot_nt(k, q) * SCALE
    if limits is not None:
        key = lax.broadcasted_iota(jnp.int32, scores.shape, 0)
        limit = jnp.where(key < rows, limits[0], limits[1] + rows)
        scores = jnp.where(key < limit, scores, -1e30)
    top = jnp.max(scores, axis=0, keepdims=True)
    raised = jnp.exp(scores - top)
    weights = raised / jnp.sum(raised, axis=0, keepdims=True)
    grad_weights = dot_nt(v, grad)
    inner = jnp.sum(weights * grad_weights, axis=0, keepdims=True)
    grad_scores = (weights * (grad_weights - inner)).astype(LOW)
    return (
        (dot_tn(grad_scores, k) * SCALE).astype(LOW),
        (jnp.dot(grad_scores, q, preferred_element_type=WIDE) * SCALE).astype(LOW),
        jnp.dot(weights.astype(LOW), grad, preferred_element_type=WIDE).astype(LOW),
    )


IN_HBM = list(
    dict(
        grad_low=0, mlp_in=0, self_mixed=0, self_in=0,
        cross_mixed=0, cross_in=0, child_in=0, mlp_up=0,
        mlp_down=0, projected=0, after_self=0, after_cross=0,
        self_project=0, cross_output=0, self_output=0, queries=0,
        keyval=0, latents=0, child_latents=0, cross_query=0,
        cross_keyval=0,
    )
)
IN_VMEM = GAINS
OUTS = list(
    dict(
        gain_out=0, parents_out=0, children_out=0, top_out=0,
    )
)
SCRATCH = list(
    dict(
        raw=0, grad=0, turned=0, act=0,
        gain_sum=0, gain_land=0, gain_part=0, proj=0,
        mix=0, stream=0, carry=0, self_low=0,
        cross_low=0, qbuf=0, w_wide=0, w_small=0,
        acc=0, back_send=0, back_land=0, top_land=0,
        load_sem=0, tile_sem=0, core_send=0, core_recv=0,
        send_sem=0, recv_sem=0, gain_send=0, gain_recv=0,
        hook_sem=0, back_ssem=0, back_rsem=0,
    )
)


def backward_kernel(plan, sources, outputs, slots, *refs):
    names = ["counts"] + IN_HBM + IN_VMEM + OUTS
    first = len(names) + len(outputs)
    refs = refs[: len(names)] + refs[first : first + len(SCRATCH)] + refs[len(names) : first] + refs[first + len(SCRATCH) :]
    names = names + SCRATCH
    r = Names(names, refs[: len(names)])
    shares = len(SHARES)
    rest = refs[len(names) :]
    totals, rest = rest[: len(outputs)], rest[len(outputs) :]
    sent, held, core_in, lands = rest[:shares], rest[shares : 2 * shares], rest[2 * shares : 3 * shares], rest[3 * shares :]
    raw, grad, turned = r.raw, r.grad, r.turned
    gain_sum, gain_land, gain_out = r.gain_sum, r.gain_land, r.gain_out
    load_sem, core_send, core_recv, send_sem, recv_sem = r.load_sem, r.core_send, r.core_recv, r.send_sem, r.recv_sem
    inner = turned.shape[2] * 2
    chunks = len(sources)
    frame, group = lax.axis_index("frames"), lax.axis_index("groups")
    rows, part, places = plan.rows, plan.part, plan.places
    halves = rows // part
    blocks = plan.frames // 2

    ids, count = {}, 0
    for i, steps in enumerate(plan.steps):
        for k in range(len(steps)):
            ids[i, k] = count
            count += 1

    def partner(kind, place):
        if kind == "f":
            return {"frames": flipped(frame, place), "groups": group}
        return {"frames": frame, "groups": flipped(group, place)}

    barrier = pltpu.get_barrier_semaphore()
    everyone = [partner("f", d) for d in range(places)] + [
        partner("g", e) for e in range(plan.group_places)
    ]
    for device in everyone:
        pl.semaphore_signal(barrier, inc=1, device_id=device, device_id_type=pl.DeviceIdType.MESH)
    pl.semaphore_wait(barrier, len(everyone))

    def core_copy(i, u):
        s = u % 2
        return pltpu.make_async_remote_copy(
            src_ref=sent[i].at[s],
            dst_ref=core_in[i].at[s],
            send_sem=core_send.at[i, s],
            recv_sem=core_recv.at[i, s],
            device_id=partner("f", 0),
            device_id_type=pl.DeviceIdType.MESH,
        )

    def step_copy(i, k, u):
        kind, place, send, _, _ = plan.steps[i][k]
        s = u % plan.lands
        return pltpu.make_async_remote_copy(
            src_ref=held[i].at[(u % slots,) + send],
            dst_ref=lands[ids[i, k]].at[s],
            send_sem=send_sem.at[ids[i, k], s],
            recv_sem=recv_sem.at[ids[i, k], s],
            device_id=partner(kind, place),
            device_id_type=pl.DeviceIdType.MESH,
        )

    def grad_load(t, which):
        right, column = sources[which][1:3]
        if right == "kvbuf":
            right, column = "act", column + 2 * inner
        return pltpu.make_async_copy(
            getattr(r, right).at[:, column : column + CHUNK], grad.at[t % 2], load_sem.at[t % 2]
        )

    def left_load(which):
        return pltpu.make_async_copy(getattr(r, sources[which][0]), raw, load_sem.at[2])

    def start_loads(which, t):
        if sources[which][1] is not None:
            grad_load(t, which).start()
        if sources[which][5] and sources[which][3] is None:
            left_load(which).start()

    def row_place(half):
        if halves == 1:
            return 0
        place = bit_of(group, 0)
        return ((1 - place) if half else place) * part

    def put_total(u, i, row, size, value):
        start, width = plan.columns[i]
        for ref, (begin, end, parts) in zip(totals, outputs):

            @pl.when((u >= begin) & (u < end))
            def _():
                at = (u - begin) // parts * rows + row
                column = (u - begin) % parts * CHUNK + start
                ref[pl.ds(pl.multiple_of(at, size), size), pl.ds(pl.multiple_of(column, 128), width)] = value

    def finish(i, k, u):
        kind, _, _, keep, _ = plan.steps[i][k]
        land = lands[ids[i, k]]
        s = u % plan.lands
        mine = held[i][(u % slots,) + keep].astype(WIDE)
        other = land[s].astype(WIDE)
        if kind == "join":
            for half, value in ((0, mine), (1, other)):
                put_total(u, i, row_place(half), part, value)
        else:
            for half in range(halves):
                own, far = half * part, (halves - 1 - half) * part
                value = mine[own : own + part] + other[far : far + part]
                put_total(u, i, row_place(half), part, value)

    def advance(i, k, u):
        step_copy(i, k, u).wait()
        if k == len(plan.steps[i]) - 1:
            finish(i, k, u)
            return
        kind, _, _, keep, _ = plan.steps[i][k]
        at = (u % slots,) + keep
        held[i][at] = held[i][at] + lands[ids[i, k]][u % plan.lands]
        step_copy(i, k + 1, u).start()

    def turn_tile(value, at):
        for piece in range(128 // part):
            slot, block, half = at(piece)
            where = xor_static(block, frame, places)
            row = (where // 2) * rows
            if halves > 1:
                row = row + xor_static(half, group, 1) * part
            row = pl.multiple_of(row, part)
            turned[slot, where % 2, pl.ds(row, part), :] = value[piece * part : (piece + 1) * part, :]

    def turn(group_of):
        stacked = group_of is not None
        per_block = r.act.shape[1] // plan.frames // 128
        for tile in range(plan.frames if stacked else inner // 128):
            if stacked:
                column = pl.multiple_of((tile * per_block + group_of) * 128, 128)
                value = r.act[:, pl.ds(column, 128)].T
            else:
                value = raw[:, tile * 128 : (tile + 1) * 128].T

            def at(piece, tile=tile):
                if stacked:
                    return piece // halves, tile, piece % halves
                run = tile * (128 // part) + piece
                return 0, run // halves, run % halves

            turn_tile(value, at)

    def any_of(t, choices):
        found = t == choices[0]
        for choice in choices[1:]:
            found = found | (t == choice)
        return found

    def make(t):
        s = t % 2
        made = [which for which in range(chunks) if sources[which][1] is None]
        loaded = [which for which in range(chunks) if sources[which][1] is not None]
        if made:

            @pl.when(t >= loaded[0])
            def _():
                grad_load(t, loaded[0]).wait()

        fresh = [which for which in range(chunks) if sources[which][5]]
        plain = [which for which in fresh if sources[which][3] is None]
        stacked = [which for which in fresh if sources[which][3] is not None]

        @pl.when(any_of(t, plain))
        def _():
            left_load(plain[0]).wait()
            turn(None)

        if stacked:

            @pl.when(any_of(t, stacked))
            def _():
                group_of = 0
                for which in stacked:
                    group_of = jnp.where(t == which, sources[which][3], group_of)
                turn(group_of)

        for which in range(1, chunks):

            @pl.when(t + 1 == which)
            def _():
                start_loads(which, t + 1)

        tslot = 0
        for which in range(chunks):
            if sources[which][4]:
                tslot = jnp.where(t == which, sources[which][4], tslot)
        for side in (1, 0):
            for i, (column, width) in enumerate(plan.columns):
                value = jnp.dot(
                    turned[tslot, side], grad[s, :, column : column + width], preferred_element_type=WIDE
                ).astype(LOW)
                size = plan.tiles[i][-2]
                for row in range(0, blocks * rows, size):
                    block, half = row // rows, row % rows // part
                    place = tuple(
                        half if kind == "cut" else (block >> (d - 1)) & 1 for kind, d in plan.axes[i]
                    )
                    target = sent[i] if side else held[i]
                    slot = s if side else t % slots
                    target[(slot,) + place] = value[row : row + size]
        for i in range(shares):
            core_copy(i, t).start()

    gain_steps = [("f", d) for d in range(places)] + [("g", e) for e in range(plan.group_places)]

    def gain_copy(k):
        return pltpu.make_async_remote_copy(
            src_ref=gain_sum,
            dst_ref=gain_land.at[k],
            send_sem=r.gain_send.at[k],
            recv_sem=r.gain_recv.at[k],
            device_id=partner(*gain_steps[k]),
            device_id_type=pl.DeviceIdType.MESH,
        )

    count = raw.shape[0]
    half_count = count // 2
    nodes, rows_each = r.parents_out.shape[0] // 2, r.parents_out.shape[1]
    features = r.parents_out.shape[2]
    side = bit_of(frame, LEVEL)
    group_heads = HEADS // 2
    units = nodes * 2
    first_self, first_cross = 2, units + 4
    first_query, first_child = 2 * units + 4, 2 * units + 6
    feeds = r.mlp_up.shape[1] // CHUNK
    when = [feeds, feeds, feeds + 1, feeds + 1, feeds + 2, feeds + 2]
    when += [feeds + i for i in (3, 4, 4, 5, 6, 7, 8, 8, 9, 10, 11)]
    first_gain = when[-1] + 1

    loads = dict(
        base=("after_self", "stream", 0),
        fed_base=("after_self", "carry", 1),
        mlp_in=("mlp_in", "mix", 14),
        grad_low=("grad_low", "cross_low", 2),
        self_output=("self_output", "w_small", 3),
        proj=("projected", "proj", 4),
        stream=("after_cross", "stream", 5),
        project=("self_project", "w_wide", 6),
        output=("cross_output", "w_small", 7),
        qbuf=("queries", "qbuf", 8),
        kvbuf=("keyval", "act", 9),
        lat=("latents", "act", 10),
        chi=("child_latents", "act", 11),
        query=("cross_query", "w_small", 12),
        keyval=("cross_keyval", "w_wide", 13),
    )

    def hook_load(name):
        source, target, place = loads[name]
        source, target = getattr(r, source), getattr(r, target)
        if source.shape != target.shape:
            start = {"chi": 1, "kvbuf": 2}.get(name, 0) * features
            target = target.at[:, start : start + source.shape[1]]
        return pltpu.make_async_copy(source, target, r.hook_sem.at[place])

    def attend_unit(unit, masked, q_ref, q_at, kv_ref, k_at, v_at):
        node, start = unit // 2, (unit % 2) * group_heads * HEAD_DIM
        own = pl.multiple_of(node * rows_each, rows_each)
        got = pl.multiple_of(half_count + node * rows_each, rows_each)

        def both(ref, column):
            columns = pl.ds(pl.multiple_of(column, HEAD_DIM), HEAD_DIM)
            return jnp.concatenate(
                [ref[pl.ds(own, rows_each), columns], ref[pl.ds(got, rows_each), columns]], axis=0
            )

        def put(ref, column, value):
            columns = pl.ds(pl.multiple_of(column, HEAD_DIM), HEAD_DIM)
            ref[pl.ds(own, rows_each), columns] = value[:rows_each]
            ref[pl.ds(got, rows_each), columns] = value[rows_each:]

        clip = side * nodes + node
        limits = None
        if masked:
            limits = (r.counts[clip, frame], r.counts[clip, flipped(frame, LEVEL)])
        for head in range(group_heads):
            at = start + head * HEAD_DIM
            places = ((q_ref, q_at + at), (kv_ref, k_at + at), (kv_ref, v_at + at))
            q, k, v = (both(*place) for place in places)
            results = attend_back_head(
                limits, rows_each, q, k, v, both(r.mix, at)
            )
            for place, result in zip(places, results):
                put(*place, result)

    def product_back_rows(ref, weight, width, half):
        start = pl.multiple_of(half * half_count, half_count)
        left = ref[pl.ds(start, half_count), 0:width]
        for column in range(0, features, 256):
            r.acc[pl.ds(start, half_count), column : column + 256] = dot_nt(
                left, weight[column : column + 256, 0:width]
            )

    def norm_back_rows(half, values_ref, gain_at, emit):
        gain = getattr(r, GAINS[gain_at])[...].astype(WIDE).reshape(1, features)
        step = 32

        def piece(i, total):
            row = pl.multiple_of(i * step, step)
            at = pl.multiple_of(half * half_count + row, step)
            values = values_ref[pl.ds(at, step), :].astype(WIDE)
            grad_out = r.acc[pl.ds(at, step), :]
            average = jnp.mean(values, axis=-1, keepdims=True)
            centred = values - average
            spread = jnp.mean(centred * centred, axis=-1, keepdims=True)
            inverse = lax.rsqrt(spread + 1e-05)
            normed = centred * inverse
            scaled = grad_out * gain
            value = inverse * (
                scaled
                - jnp.mean(scaled, axis=-1, keepdims=True)
                - normed * jnp.mean(scaled * normed, axis=-1, keepdims=True)
            )
            emit(row, at, value)
            share = grad_out * normed
            for top in range(0, step, 8):
                total = total + share[top : top + 8]
            return total

        zero = jnp.zeros((8, features), WIDE)
        total = lax.fori_loop(0, half_count // step, piece, zero)
        r.gain_part[gain_at] = jnp.where(half == 0, zero, r.gain_part[gain_at]) + total

    def swap_copy(which):
        return pltpu.make_async_remote_copy(
            src_ref=r.back_send.at[which],
            dst_ref=r.back_land.at[which],
            send_sem=r.back_ssem.at[which],
            recv_sem=r.back_rsem.at[which],
            device_id=partner("f", LEVEL),
            device_id_type=pl.DeviceIdType.MESH,
        )

    def top_copy():
        return pltpu.make_async_remote_copy(
            src_ref=r.back_send.at[0],
            dst_ref=r.top_land,
            send_sem=r.back_ssem.at[2],
            recv_sem=r.back_rsem.at[2],
            device_id=partner("f", LEVEL),
            device_id_type=pl.DeviceIdType.MESH,
        )

    def emit_last(which, out, carried):
        def emit(row, at, value):
            total = value + r.carry[pl.ds(at, 32), :] if carried else value
            node = row // rows_each
            inside = pl.multiple_of(row % rows_each, 32)

            @pl.when(at < half_count)
            def _():
                out[side * nodes + node, pl.ds(inside, 32), :] = total.astype(LOW)

            @pl.when(at >= half_count)
            def _():
                r.back_send[which, pl.ds(row, 32), :] = total.astype(LOW)

        return emit

    def arrived(which, out):
        swap_copy(which).wait()
        for node in range(nodes):
            out[(1 - side) * nodes + node] = r.back_land[
                which, node * rows_each : (node + 1) * rows_each, :
            ]

    def wait_for(t, when, *which):
        @pl.when(t == when)
        def _():
            for name in which:
                hook_load(name).wait()

    def hook(t):
        def mix_rows(source, half):
            start = pl.multiple_of(half * half_count, half_count)
            left = source[pl.ds(start, half_count), :]
            for column in range(0, features, 256):
                r.mix[pl.ds(start, half_count), column : column + 256] = dot_nt(
                    left, r.w_small[column : column + 256, :]
                ).astype(LOW)

        wait_for(t, 0, "base", "self_output")

        @pl.when(t < first_self)
        def _():
            def emit(row, at, value):
                total = r.cross_low[pl.ds(at, 32), :].astype(WIDE) + value
                r.carry[pl.ds(at, 32), :] = total
                r.self_low[pl.ds(at, 32), :] = total.astype(LOW)

            norm_back_rows(t, r.stream, 3, emit)
            mix_rows(r.self_low, t)

        @pl.when(t == first_self - 1)
        def _():
            hook_load("stream").start()
            hook_load("output").start()

        wait_for(t, first_self, "proj")

        @pl.when((t >= first_self) & (t < first_self + units))
        def _():
            attend_unit(t - first_self, False, r.proj, 0, r.proj, features, 2 * features)

        first_middle = first_self + units
        wait_for(t, first_middle, "stream", "project", "output")

        @pl.when((t >= first_middle) & (t < first_middle + 2))
        def _():
            half = t - first_middle
            product_back_rows(r.proj, r.w_wide, 3 * features, half)

            def emit(row, at, value):
                total = r.carry[pl.ds(at, 32), :] + value
                r.carry[pl.ds(at, 32), :] = total
                r.cross_low[pl.ds(at, 32), :] = total.astype(LOW)

            norm_back_rows(half, r.stream, 2, emit)
            mix_rows(r.cross_low, half)

        @pl.when(t == first_middle + 1)
        def _():
            hook_load("query").start()
            hook_load("keyval").start()

        wait_for(t, first_cross, "qbuf", "kvbuf")

        @pl.when((t >= first_cross) & (t < first_cross + units))
        def _():
            attend_unit(t - first_cross, True, r.qbuf, 0, r.act, 2 * features, 3 * features)

        wait_for(t, first_query, "query", "lat")

        @pl.when((t >= first_query) & (t < first_query + 2))
        def _():
            half = t - first_query
            product_back_rows(r.qbuf, r.w_small, features, half)
            norm_back_rows(half, r.act.at[:, 0:features], 1, emit_last(0, r.parents_out, True))

        wait_for(t, first_child, "keyval", "chi")

        @pl.when((t >= first_child) & (t < first_child + 2))
        def _():
            half = t - first_child
            product_back_rows(r.act.at[:, 2 * features : 4 * features], r.w_wide, 2 * features, half)
            norm_back_rows(half, r.act.at[:, features : 2 * features], 0, emit_last(1, r.children_out, False))

        @pl.when(t == first_query + 2)
        def _():
            swap_copy(0).start()

        @pl.when(t == first_child + 2)
        def _():
            swap_copy(1).start()

        @pl.when(t == len(when) - 1)
        def _():
            for i in range(4):
                gain_sum[i : i + 1, :] = jnp.sum(r.gain_part[i], axis=0, keepdims=True)
            gain_sum[4:8, :] = jnp.zeros((4, features), WIDE)

    last = max(chunks + plan.lag * plan.depth, first_gain + len(gain_steps) + 1)

    turned_by = max([0] + [which for which in range(chunks) if sources[which][5] and sources[which][3] is not None])

    def last_hook(t):
        @pl.when(t == turned_by)
        def _():
            hook_load("lat").start()
            hook_load("chi").start()
            hook_load("kvbuf").start()

        @pl.when(t == feeds + 5)
        def _():
            top_copy().wait()
            for node in range(nodes):
                r.top_out[(1 - side) * nodes + node] = r.top_land[
                    node * rows_each : (node + 1) * rows_each, :
                ]


        @pl.when(t == last - 1)
        def _():
            arrived(0, r.parents_out)

        @pl.when(t == last)
        def _():
            arrived(1, r.children_out)

    def gain_work(t):
        for k in range(len(gain_steps) + 1):

            @pl.when(t == first_gain + k + 1)
            def _():
                if k:
                    gain_copy(k - 1).wait()
                    gain_sum[...] = gain_sum[...] + gain_land[k - 1]
                if k < len(gain_steps):
                    gain_copy(k).start()
                else:
                    gain_out[...] = gain_sum[...]

    def tile_loads(tile):
        slot = tile % 2
        column = pl.multiple_of(tile * FEED, FEED)
        place = pl.ds(pl.multiple_of(slot * FEED, FEED), FEED)
        return (
            pltpu.make_async_copy(
                r.mlp_up.at[:, pl.ds(column, FEED)], r.w_wide.at[:, place], r.tile_sem.at[0, slot]
            ),
            pltpu.make_async_copy(
                r.mlp_down.at[pl.ds(column, FEED), :], r.w_small.at[place, :], r.tile_sem.at[1, slot]
            ),
        )

    tiles = r.mlp_up.shape[1] // FEED
    per_chunk = CHUNK // FEED

    def feed(t):
        @pl.when(t == 0)
        def _():
            for name in ("mlp_in", "grad_low", "fed_base"):
                hook_load(name).wait()
            r.acc[...] = jnp.zeros_like(r.acc)

        def one(i, carry):
            tile = t * per_chunk + i
            for copy in tile_loads(tile):
                copy.wait()
            place = pl.ds(pl.multiple_of(tile % 2 * FEED, FEED), FEED)
            column = pl.ds(pl.multiple_of(tile * FEED, FEED), FEED)
            up, down = r.w_wide[:, place], r.w_small[place, :]
            for half in (0, 1):
                here = slice(half * half_count, (half + 1) * half_count)
                hidden = jnp.dot(r.mix[here, :], up, preferred_element_type=WIDE)
                grad_act = dot_nt(r.cross_low[here, :], down)
                normal = 0.5 * (1.0 + lax.erf(hidden * 0.7071067811865476))
                density = jnp.exp(-0.5 * hidden * hidden) * 0.3989422804014327
                act = (hidden * normal).astype(LOW)
                grad_hidden = (grad_act * (normal + hidden * density)).astype(LOW)
                r.act[here, column] = act
                grad[t % 2, here, pl.ds(pl.multiple_of(i * FEED, FEED), FEED)] = grad_hidden
                r.carry[here, :] += jnp.dot(act, down, preferred_element_type=WIDE)
                r.acc[here, :] += dot_nt(grad_hidden, up)

            @pl.when(tile + 2 < tiles)
            def _():
                for copy in tile_loads(tile + 2):
                    copy.start()

            return carry

        lax.fori_loop(0, per_chunk, one, 0)

        @pl.when(t == feeds - 1)
        def _():
            hook_load("self_output").start()
            hook_load("project").start()
            for node in range(nodes):
                mine = slice(node * rows_each, (node + 1) * rows_each)
                r.top_out[side * nodes + node] = r.carry[mine, :].astype(LOW)
            r.back_send[0] = r.carry[half_count:, :].astype(LOW)
            top_copy().start()

    for name in ("mlp_in", "grad_low", "fed_base"):
        hook_load(name).start()
    for tile in (0, 1):
        for copy in tile_loads(tile):
            copy.start()
    start_loads(0, 0)
    for name in ["base", "proj", "qbuf"]:
        hook_load(name).start()

    def iteration(t, carry):
        for k in reversed(range(plan.depth)):
            u = t - 1 - plan.lag * (k + 1)

            @pl.when((u >= 0) & (u < chunks))
            def _():
                for i in range(len(plan.steps)):
                    if k < len(plan.steps[i]):
                        advance(i, k, u)

        u = t - 1

        @pl.when((u >= 0) & (u < chunks))
        def _():
            for i in range(shares):
                core_copy(i, u).wait()
                here = u % slots
                held[i][here] = held[i][here] + core_in[i][u % 2]
                step_copy(i, 0, u).start()

        @pl.when(t < feeds)
        def _():
            feed(t)

        @pl.when(t < chunks)
        def _():
            make(t)

        def piece(h, inner_carry):
            hook(h)
            return inner_carry

        begin = end = 0
        for place in when:
            begin = begin + jnp.where(t > place, 1, 0)
            end = end + jnp.where(t >= place, 1, 0)
        lax.fori_loop(begin, end, piece, 0)

        last_hook(t)
        gain_work(t)
        return carry

    lax.fori_loop(0, last + 1, iteration, 0)


def backward(values, counts, clips, frames, groups):
    pairs = [
        ("mlp_in", None, 4),
        ("act", "grad_low", 1),
        ("self_mixed", "self_low", 1),
        ("self_in", "proj", 3),
        ("cross_mixed", "cross_low", 1),
        ("cross_in", "qbuf", 1),
        ("child_in", "kvbuf", 2),
    ]
    count, features = values["mlp_in"].shape
    hidden = values["mlp_up"].shape[1]
    plan = Plan(frames, groups, features)
    per_tile = max(1, 128 // plan.rows)
    slots = plan.lag * plan.depth + 1
    steps = [step for steps in plan.steps for step in steps]
    gain_steps = plan.places + plan.group_places
    half_count, nodes = count // 2, clips // 2
    rows_each = half_count // nodes
    vmem, dma = pltpu.VMEM, pltpu.SemaphoreType.DMA
    scratch = dict(
        raw=vmem((count, features), LOW),
        act=vmem((count, hidden), LOW),
        grad=vmem((2, count, CHUNK), LOW),
        turned=vmem((per_tile, 2, features // 2, count), LOW),
        gain_sum=vmem((8, features), WIDE),
        gain_land=vmem((gain_steps, 8, features), WIDE),
        gain_part=vmem((4, 8, features), WIDE),
        proj=vmem((count, 3 * features), LOW),
        mix=vmem((count, features), LOW),
        stream=vmem((count, features), WIDE),
        carry=vmem((count, features), WIDE),
        self_low=vmem((count, features), LOW),
        cross_low=vmem((count, features), LOW),
        qbuf=vmem((count, features), LOW),
        w_wide=vmem((features, 3 * features), LOW),
        w_small=vmem((features, features), LOW),
        acc=vmem((count, features), WIDE),
        back_send=vmem((2, half_count, features), LOW),
        back_land=vmem((2, half_count, features), LOW),
        top_land=vmem((half_count, features), LOW),
        load_sem=dma((3,)),
        tile_sem=dma((2, 2)),
        core_send=dma((len(SHARES), 2)),
        core_recv=dma((len(SHARES), 2)),
        send_sem=dma((len(steps), plan.lands)),
        recv_sem=dma((len(steps), plan.lands)),
        gain_send=dma((gain_steps,)),
        gain_recv=dma((gain_steps,)),
        hook_sem=dma((15,)),
        back_ssem=dma((3,)),
        back_rsem=dma((3,)),
    )
    in_vmem = pl.BlockSpec(memory_space=vmem)
    clip_shape = (clips, rows_each, features)
    sources, layout = [], []
    for left, right, _ in pairs:
        ref = values["keyval"] if right == "kvbuf" else values.get(right, scratch.get(right, values["mlp_up"]))
        wide = ref.shape[1]
        stack = (hidden if left == "act" else features) // features
        if stack > 1:
            layout.append((stack, wide // CHUNK))
            for i in range(stack):
                for column in range(0, wide, CHUNK):
                    new = i % per_tile == 0 and column == 0
                    sources.append((left, right, column, i // per_tile, i % per_tile, new))
        else:
            layout.append((1, wide // CHUNK))
            for column in range(0, wide, CHUNK):
                sources.append((left, right, column, None, 0, column == 0))
    chunks = len(sources)
    outputs, at = [], 0
    for stack, parts in layout:
        outputs.append((at, at + stack * parts, parts))
        at += stack * parts
    gain_total, parents_out, children_out, top_out, *outs = pl.pallas_call(
        partial(backward_kernel, plan, sources, outputs, slots),
        out_shape=[
            jax.ShapeDtypeStruct((8, features), WIDE),
            jax.ShapeDtypeStruct(clip_shape, LOW),
            jax.ShapeDtypeStruct(clip_shape, LOW),
            jax.ShapeDtypeStruct(clip_shape, LOW),
        ]
        + [
            jax.ShapeDtypeStruct((stack * plan.rows, parts * CHUNK), WIDE) for stack, parts in layout
        ],
        in_specs=[pl.BlockSpec(memory_space=pltpu.SMEM)]
        + [pl.BlockSpec(memory_space=pl.ANY)] * len(IN_HBM)
        + [in_vmem] * len(IN_VMEM),
        out_specs=[in_vmem] * (4 + len(layout)),
        scratch_shapes=[scratch[name] for name in SCRATCH]
        + [vmem((n,) + tile, LOW) for n in (2, slots, 2) for tile in plan.tiles]
        + [vmem((plan.lands,) + step[-1], LOW) for step in steps],
        compiler_params=pltpu.CompilerParams(
            collective_id=0, has_side_effects=True, vmem_limit_bytes=67043328
        ),
        cost_estimate=pl.CostEstimate(
            flops=2 * count * features * CHUNK * chunks * 5,
            bytes_accessed=4 * count * CHUNK * chunks,
            transcendentals=0,
        ),
        name="backward",
    )(counts, *[values[name] for name in IN_HBM + IN_VMEM])
    return outs, gain_total, parents_out.astype(WIDE), children_out.astype(WIDE), top_out


def body(
    parents,
    children,
    child_counts,
    out_grad,
    child_gain,
    cross_gain,
    cross_query,
    cross_keyval,
    cross_output,
    self_gain,
    self_project,
    self_output,
    mlp_gain,
    mlp_up,
    mlp_down,
):
    clips, _, features = parents.shape
    frames, groups = lax.axis_size("frames"), lax.axis_size("groups")
    frame = lax.axis_index("frames")
    values = dict(
        parents=parents,
        children=children,
        out_grad=out_grad,
        child_gain=child_gain,
        cross_gain=cross_gain,
        self_gain=self_gain,
        mlp_gain=mlp_gain,
        cross_query=cross_query,
        cross_keyval=cross_keyval,
        cross_output=cross_output,
        self_project=self_project,
        self_output=self_output,
    )
    values.update(forward(child_counts, values))
    values.update(
        mlp_up=mlp_up, mlp_down=mlp_down, latents=values["parent_low"], child_latents=values["child_low"]
    )
    totals, gains, grad_parents, grad_children, top_latents = backward(
        values, child_counts, clips, frames, groups
    )
    total_up, total_down, total_self_out, total_project, total_cross_out, total_query, total_keyval = totals
    width = features // frames
    gains = lax.dynamic_slice_in_dim(gains, frame * width, width, 1)
    return (
        top_latents,
        grad_parents,
        grad_children,
        gains[0],
        gains[1],
        total_query,
        total_keyval,
        total_cross_out,
        gains[2],
        total_project,
        total_self_out,
        gains[3],
        total_up,
        total_down,
    )


def solution(mesh):
    rows = P("groups", "frames", None)
    shard, shard2 = P("frames"), P("frames", None)
    return jax.shard_map(
        body,
        mesh=mesh,
        in_specs=(rows, rows, P("groups", None), rows) + (P(),) * 11,
        out_specs=(
            rows,
            rows,
            rows,
            shard,
            shard,
            shard2,
            shard2,
            shard2,
            shard,
            shard2,
            shard2,
            shard,
            shard2,
            shard2,
        ),
        check_vma=False,
    )
```
